512 devices in a mesh: grp: 2 (over y), shot: 16 (over x, core), slab: 16 (over z).
Axes of the slice: x: 8, y: 2, z: 16, core: 2. Of those that a mesh axis runs over, the one named last changes fastest.
The devices are a block of a 8x8x16 slice.
Arguments:
- courant_sq: float32 [2048, 1024], P(('grp', 'slab')), parts along dimension 0, may hold values from 0.05 to 0.25
- sponge_level: int32 [2048, 1024], P(('grp', 'slab')), parts along dimension 0, may hold values from 0 to 3
- source_later: float32 [64, 1024, 1024], P(('grp', 'shot'), 'slab'), parts along dimension 0, may hold values from -6 to 6
- source_now: float32 [64, 1024, 1024], P(('grp', 'shot'), 'slab'), parts along dimension 0, may hold values from -6 to 6
- receiver_later: float32 [64, 1024, 1024], P(('grp', 'shot'), 'slab'), parts along dimension 0, may hold values from -6 to 6
- receiver_now: float32 [64, 1024, 1024], P(('grp', 'shot'), 'slab'), parts along dimension 0, may hold values from -6 to 6
- traces: float32 [64, 16, 512], P(('grp', 'shot')), parts along dimension 0, may hold values from -24 to 24
- wavelet: float32 [512], P('grp'), parts along dimension 0, may hold values from -24 to 24
- source_depth: int32 [64], P(('grp', 'shot')), parts along dimension 0, may hold values from 0 to 1023
- source_lateral: int32 [64], P(('grp', 'shot')), parts along dimension 0, may hold values from 0 to 1023
- receiver_depth: int32 [64, 512], P(('grp', 'shot')), parts along dimension 0, may hold values from 0 to 1023
- receiver_lateral: int32 [64, 512], P(('grp', 'shot')), parts along dimension 0, may hold values from 0 to 1023
- checkpoint_step: int32 [64], P(('grp', 'shot')), parts along dimension 0, may hold values from 0 to 240
Outputs:
- image: float32 [2048, 1024], P(('grp', 'slab')), parts along dimension 0
- source_out: float32 [64, 1024, 1024], P(('grp', 'shot'), 'slab'), parts along dimension 0
- receiver_out: float32 [64, 1024, 1024], P(('grp', 'shot'), 'slab'), parts along dimension 0
The draws below stay inside these ranges and needn't reach their ends.
There are 2 independent parts, one for each index of `grp`. The reference program is written for one: setup_inputs(seed, part) draws one part's arguments, and reference() takes and returns one part's arrays. A program takes and returns all parts, laid end to end along the dimension named above; each array names one. Nothing has to cross between parts.
All inputs are finite; a program needn't handle non-finite values.
Results may differ from the reference program's by a relative error of at most 0.0003.
Values sent between devices are 32-bit elements; how exact they have to be, the bound alone decides.
A program may use at most 64 MiB of HBM per device.

```python
import math
import jax
import jax.numpy as jnp
from jax import lax

NX = 1024
STEPS = 16
NREC = 512
NT = 256
NZ = 1024
SHOTS = 32


def with_ends(drawn, stream_key, smallest, largest):
    dims = drawn.shape
    place = [jax.random.randint(jax.random.fold_in(stream_key, axis), (), 0, dims[axis]) for axis in range(len(dims))]
    drawn = drawn.at[tuple(place)].set(smallest)
    longest = dims.index(max(dims))
    place[longest] = (place[longest] + 1) % dims[longest]
    return drawn.at[tuple(place)].set(largest)


def level_of(key, shape, split, least, top_value):
    factor_of, own = 1.0, jax.random.fold_in(key, 6)
    for position, shards_of in split:
        steps = jnp.exp(jax.random.uniform(jax.random.fold_in(own, position), (shards_of,), jnp.float32, least / len(split), top_value / len(split)))
        factor_of = factor_of * jnp.repeat(steps, shape[position] // shards_of).reshape([-1 if axis == position else 1 for axis in range(len(shape))])
    return factor_of


def normal_values(key, dims, spread, most, split=(), kind=jnp.bfloat16):
    values = spread * jax.random.normal(key, dims, jnp.float32)
    if split:
        values = values * level_of(key, dims, split, -0.22, 0.18)
    return jnp.clip(values, -most, most).astype(kind)


def setup_inputs(seed: int = 0, part: int = 0) -> dict:
    streams_of = jax.random.split(jax.random.key(seed), 14)
    own_keys = jax.random.split(jax.random.fold_in(streams_of[13], part), 14)
    return {
        "courant_sq": jnp.clip(jnp.exp(math.log(0.25) - 1.609438 * jax.random.uniform(own_keys[0], (NZ, NX), jnp.float32) ** level_of(own_keys[0], (NZ, NX), ((0, 16),), -0.2, 0.2)), 0.05, 0.25),
        "sponge_level": with_ends(jax.random.randint(own_keys[1], (NZ, NX), 0, 4), jax.random.fold_in(own_keys[1], 1), 0, 3).astype(jnp.int32),
        "source_later": normal_values(own_keys[2], (SHOTS, NZ, NX), 1.0, 6.0, ((0, 16), (1, 16)), jnp.float32),
        "source_now": normal_values(own_keys[3], (SHOTS, NZ, NX), 1.0, 6.0, ((0, 16), (1, 16)), jnp.float32),
        "receiver_later": normal_values(own_keys[4], (SHOTS, NZ, NX), 1.0, 6.0, ((0, 16), (1, 16)), jnp.float32),
        "receiver_now": normal_values(own_keys[5], (SHOTS, NZ, NX), 1.0, 6.0, ((0, 16), (1, 16)), jnp.float32),
        "traces": normal_values(own_keys[6], (SHOTS, STEPS, NREC), 4.0, 24.0, ((0, 16),), jnp.float32),
        "wavelet": normal_values(own_keys[7], (NT,), 4.0, 24.0, (), jnp.float32),
        "source_depth": with_ends(jax.random.randint(own_keys[8], (SHOTS,), 0, NZ), jax.random.fold_in(own_keys[8], 1), 0, NZ - 1).astype(jnp.int32),
        "source_lateral": with_ends(jax.random.randint(own_keys[9], (SHOTS,), 0, NX), jax.random.fold_in(own_keys[9], 1), 0, NX - 1).astype(jnp.int32),
        "receiver_depth": with_ends(jax.random.randint(own_keys[10], (SHOTS, NREC), 0, NZ), jax.random.fold_in(own_keys[10], 1), 0, NZ - 1).astype(jnp.int32),
        "receiver_lateral": with_ends(jax.random.randint(own_keys[11], (SHOTS, NREC), 0, NX), jax.random.fold_in(own_keys[11], 1), 0, NX - 1).astype(jnp.int32),
        "checkpoint_step": with_ends(jax.random.randint(own_keys[12], (SHOTS,), 0, NT - STEPS + 1), jax.random.fold_in(own_keys[12], 1), 0, NT - STEPS).astype(jnp.int32),
    }


stencil_coeffs = (-205.0 / 72.0, 8.0 / 5.0, -1.0 / 5.0, 8.0 / 315.0, -1.0 / 560.0)

def laplace(extended):
    row_count = extended.shape[-2] - 8
    width = extended.shape[-1]
    centre = extended[..., 4:4 + row_count, :]
    pad_spec = [(0, 0)] * (centre.ndim - 1) + [(4, 4)]
    padded = jnp.pad(centre, pad_spec)
    result = 2.0 * stencil_coeffs[0] * centre
    for offset in range(1, 5):
        result = result + stencil_coeffs[offset] * (extended[..., 4 + offset:4 + offset + row_count, :] + extended[..., 4 - offset:4 - offset + row_count, :] + padded[..., 4 + offset:4 + offset + width] + padded[..., 4 - offset:4 - offset + width])
    return result

def reference(courant_sq, sponge_level, source_later, source_now, receiver_later, receiver_now, traces, wavelet, source_depth, source_lateral, receiver_depth, receiver_lateral, checkpoint_step):
    damping = 1.0 - 0.06 * sponge_level.astype(jnp.float32)

    def one_shot(image_sum, items):
        src_hi, src_now, rec_hi, rec_now, shot_traces, depth_src, lateral_src, depth_rec, lateral_rec, start = items
        for step_index in range(STEPS):
            image_sum = image_sum + src_now * rec_now
            both = jnp.pad(jnp.stack([src_now, rec_now]), ((0, 0), (4, 4), (0, 0)))
            laplacian = laplace(both)
            pulse = wavelet[start + STEPS - 1 - step_index]
            src_next = 2.0 * src_now - src_hi + courant_sq * laplacian[0]
            src_next = src_next.at[depth_src, lateral_src].add(-(courant_sq[depth_src, lateral_src] * pulse))
            rec_next = 2.0 * rec_now - rec_hi + courant_sq * laplacian[1]
            rec_next = rec_next.at[depth_rec, lateral_rec].add(courant_sq[depth_rec, lateral_rec] * shot_traces[step_index])
            rec_next = damping * rec_next
            src_hi, src_now, rec_hi, rec_now = (src_now, src_next, rec_now, rec_next)
        return (image_sum, (src_now, rec_now))
    start_image = jnp.zeros(courant_sq.shape, jnp.float32)
    image_sum, (source_out, receiver_out) = lax.scan(one_shot, start_image, (source_later, source_now, receiver_later, receiver_now, traces, source_depth, source_lateral, receiver_depth, receiver_lateral, checkpoint_step))
    image = image_sum / math.sqrt(STEPS * SHOTS)
    return (image, source_out, receiver_out)
```

```python
import functools
import math

import jax
import jax.numpy as jnp
from jax import lax
from jax.experimental import pallas as pl
from jax.experimental.pallas import tpu as pltpu
from jax.sharding import PartitionSpec as P

MESH = pl.DeviceIdType.MESH
F32 = jnp.float32
BF16 = jnp.bfloat16

C0, C1, C2, C3, C4 = (-205.0 / 72.0, 8.0 / 5.0, -1.0 / 5.0, 8.0 / 315.0, -1.0 / 560.0)

OWN = slice(4, 12)


def rows(start, count=8):
    return pl.ds(start, count)


def kernel(
    steps,
    courant,
    sponge,
    src_hi,
    src_now,
    rec_hi,
    rec_now,
    traces,
    rec_depth,
    rec_lateral,
    wavelet,
    src_depth,
    src_lateral,
    start_step,
    image_out,
    src_out,
    rec_out,
    N,
    M,
    V,
    D,
    AS,
    VS,
    AR,
    VR,
    G,
    IA,
    IB,
    W,
    DP,
    T,
    CORR,
    PAIR,
    HALF,
    PARTS,
    FIN,
    IMG,
    n_send,
    n_recv,
    h_send,
    h_recv,
    c_send,
    c_recv,
    pair_send,
    pair_recv,
    rs_send,
    rs_recv,
    ag_send,
    ag_recv,
):
    slab, slabs = lax.axis_index("slab"), lax.axis_size("slab")
    me, members = lax.axis_index("shot"), lax.axis_size("shot")
    chips = members // 2
    chip, core = me // 2, lax.rem(me, 2)
    depth = courant.shape[0]
    shots = src_now.shape[0]
    nrec = traces.shape[2]
    blocks = steps // 2
    wide = depth + 8
    first = slab * depth
    has_up, has_down = slab > 0, slab < slabs - 1
    part = depth // chips
    planes = 2 * shots

    barrier = pltpu.get_barrier_semaphore()

    def greet(target):
        pl.semaphore_signal(barrier, inc=1, device_id=target, device_id_type=MESH)

    @pl.when(has_up)
    def _():
        greet({"slab": slab - 1})

    @pl.when(has_down)
    def _():
        greet({"slab": slab + 1})

    partner = chip * 2 + (1 - core)
    greet({"shot": partner})
    peers = [lax.rem(chip + d, chips) * 2 + core for d in range(1, chips)]
    for peer in peers:
        greet({"shot": peer})

    lane = lax.broadcasted_iota(jnp.int32, (4, 8, 128), 2)
    lane8 = lax.broadcasted_iota(jnp.int32, (8, 8, 128), 2)
    reg8 = lax.broadcasted_iota(jnp.int32, (8, 8, 128), 0)
    row8 = lax.broadcasted_iota(jnp.int32, (8, 8, 128), 1)
    cell8 = 8 * lane8 + reg8

    def up_lane(v):
        return jnp.where(lane == 0, 0.0, pltpu.roll(v, 1, axis=2))

    def down_lane(v):
        return jnp.where(lane == 127, 0.0, pltpu.roll(v, 127, axis=2))

    def to_registers(block, slot, put):
        for t in range(8):
            T[slot, 128 * t : 128 * (t + 1), :] = block(t).T
        for r in range(8):
            put(r, T[slot, pl.ds(r, 128, stride=8), :].T)

    def field_block(ref):
        return lambda t: ref[:, :, 128 * t : 128 * (t + 1)].reshape(shots * depth, 128)

    def put_now(field):
        def put(r, value):
            for s in range(shots):
                v = value[depth * s : depth * (s + 1)]
                N[0, 2 * s + field, 4 + r, 8 : 8 + depth, :] = v
                edge = lax.broadcasted_iota(jnp.int32, (depth, 128), 1)
                if r < 4:
                    N[0, 2 * s + field, 12 + r, 8 : 8 + depth, :] = jnp.where(
                        edge == 127, 0.0, pltpu.roll(v, 127, axis=1)
                    )
                else:
                    N[0, 2 * s + field, r - 4, 8 : 8 + depth, :] = jnp.where(
                        edge == 0, 0.0, pltpu.roll(v, 1, axis=1)
                    )

        return put

    def put_hi(field):
        def put(r, value):
            for s in range(shots):
                M[2 * s + field, 4 + r, 4 : 4 + depth, :] = value[depth * s : depth * (s + 1)]

        return put

    def model_block(t):
        cols = slice(128 * t, 128 * (t + 1))
        return jnp.concatenate(
            [courant[:, cols], 1.0 - 0.06 * sponge[:, cols].astype(F32)], axis=0
        )

    def put_model(r, value):
        V[r, 4 : 4 + depth, :] = value[:depth]
        D[r, 4 : 4 + depth, :] = value[depth:]

    zeros = jnp.zeros((8, 8, 128), F32)

    def clear(now_row, row):
        for p in range(planes):
            for slot in range(2):
                N[slot, p, OWN, rows(now_row), :] = zeros
            M[p, OWN, rows(row), :] = zeros
        for ref in (V, D):
            ref[:, rows(row), :] = zeros

    @pl.when(slab == 0)
    def _():
        clear(0, 0)

    @pl.when(slab == slabs - 1)
    def _():
        clear(8 + depth, depth)

    to_registers(field_block(src_now), 0, put_now(0))
    to_registers(field_block(src_hi), 1, put_hi(0))
    to_registers(field_block(rec_now), 0, put_now(1))
    to_registers(field_block(rec_hi), 1, put_hi(1))
    to_registers(model_block, 0, put_model)

    def shift(ref_at, src_row, dst_row, count, send, recv, to):
        return pltpu.make_async_remote_copy(
            src_ref=ref_at(src_row, count),
            dst_ref=ref_at(dst_row, count),
            send_sem=send,
            recv_sem=recv,
            device_id={"slab": to},
            device_id_type=MESH,
        )

    def now_copy(slot, p, direction):
        at = lambda row, count: N.at[slot, p, OWN, pl.ds(row, count), :]
        if direction == 0:
            return shift(at, 8, 8 + depth, 8, n_send.at[p, 0], n_recv.at[slot, p, 0], slab - 1)
        return shift(at, depth, 0, 8, n_send.at[p, 1], n_recv.at[slot, p, 1], slab + 1)

    def hi_copy(p, direction):
        at = lambda row, count: M.at[p, OWN, pl.ds(row, count), :]
        if direction == 0:
            return shift(at, 4, 4 + depth, 4, h_send.at[p, 0], h_recv.at[p, 0], slab - 1)
        return shift(at, depth, 0, 4, h_send.at[p, 1], h_recv.at[p, 1], slab + 1)

    def model_copy(which, direction):
        ref = (V, D)[which]
        at = lambda row, count: ref.at[:, pl.ds(row, count), :]
        sems = c_send.at[which, direction], c_recv.at[which, direction]
        if direction == 0:
            return shift(at, 4, 4 + depth, 4, *sems, slab - 1)
        return shift(at, depth, 0, 4, *sems, slab + 1)

    def each_way(act):
        @pl.when(has_up)
        def _():
            act(0, 1)

        @pl.when(has_down)
        def _():
            act(1, 0)

    greeted = (
        has_up.astype(jnp.int32) + has_down.astype(jnp.int32) + len(peers) + 1
    )
    pl.semaphore_wait(barrier, greeted)

    def send_first(out, _):
        model_copy(0, out).start()
        model_copy(1, out).start()
        for p in range(planes):
            hi_copy(p, out).start()
            now_copy(0, p, out).start()

    each_way(send_first)

    pad = 16 * ((wide + 15) // 16)
    top = 2 * pad

    rec_ids = first - 4 + lax.broadcasted_iota(jnp.int32, (wide, nrec), 0)
    for s in range(shots):
        DP[s] = (rec_ids == rec_depth[s : s + 1, :]).astype(F32)
        for q in range(nrec // 128):
            wanted = jnp.broadcast_to(
                rec_lateral[s : s + 1, 128 * q : 128 * (q + 1)].astype(F32), (128, 128)
            ).T
            at = lax.broadcasted_iota(jnp.int32, (128, 128), 1).astype(F32) * 8.0
            for r in range(8):
                W[s, 128 * q : 128 * (q + 1), 128 * r : 128 * (r + 1)] = (
                    (wanted == at + float(r)).astype(F32).astype(BF16)
                )

    def inject(s, block):
        def terms(step):
            t = traces[s, pl.ds(step, 1), :] * (1.0 / C1)
            hi = t.astype(BF16).astype(F32)
            return hi, t - hi

        gap = jnp.zeros((pad - wide, nrec), F32)
        table = []
        for term in terms(2 * block):
            table += [DP[s] * term, gap]
        for term in terms(2 * block + 1):
            table += [DP[s, 4 : 4 + depth, :] * term]
        table = jnp.concatenate(table, axis=0).astype(BF16)
        for c in range(4):
            got = jnp.dot(
                table, W[s, :, 256 * c : 256 * (c + 1)], preferred_element_type=F32
            )
            a = got[0:wide] + got[pad : pad + wide]
            b = got[top : top + depth] + got[top + depth : top + 2 * depth]
            for e in range(2):
                IA[s, 2 * c + e] = a[:, 128 * e : 128 * (e + 1)]
                IB[s, 2 * c + e] = b[:, 128 * e : 128 * (e + 1)]

    def coefficients(m):
        at = rows(m)
        v, d = V[:, at, :], D[:, at, :]
        a = 2.0 + (2.0 * C0) * v
        AS[:, at, :] = a
        AR[:, at, :] = d * a
        VS[:, at, :] = C1 * v
        VR[:, at, :] = (C1 * d) * v
        for s in range(shots):
            hit = (cell8 == src_lateral[s]) & (row8 + (first - 4 + m) == src_depth[s])
            G[s, :, at, :] = jnp.where(hit, -v, 0.0)

    def spread(X, z):
        total = None
        for k, a in ((1, None), (2, C2 / C1), (3, C3 / C1), (4, C4 / C1)):
            pair = (X(4 + k) + X(4 - k)) + (z(k) + z(-k))
            total = pair if a is None else total + a * pair
        return total

    def neighbours(ref, pre, row, stored):
        z = lambda k: ref[pre + (OWN, rows(row + k), slice(None))]
        if stored:
            X = lambda k: ref[pre + (slice(k, k + 8), rows(row), slice(None))]
            return X, z
        c = z(0)
        wide_c = jnp.concatenate([up_lane(c[4:]), c, down_lane(c[:4])], axis=0)
        return (lambda k: wide_c[k : k + 8]), z

    def advance(field, s, centre, total, hi, m, injected, pulse):
        at = rows(m)
        if field == 0:
            return AS[:, at, :] * centre - hi + (VS[:, at, :] * total + pulse * G[s, :, at, :])
        return AR[:, at, :] * centre - D[:, at, :] * hi + VR[:, at, :] * (total + injected)

    def put_field(ref, pre, row, value):
        at = rows(row)
        ref[pre + (OWN, at, slice(None))] = value
        ref[pre + (slice(12, 16), at, slice(None))] = down_lane(value[:4])
        ref[pre + (slice(0, 4), at, slice(None))] = up_lane(value[4:])

    def first_step(slot, s, field, g, pulse, stored):
        p, m = 2 * s + field, 8 * g
        X, z = neighbours(N, (slot, p), m + 4, stored)
        injected = IA[s, :, rows(m), :] if field else None
        new = advance(field, s, z(0), spread(X, z), M[p, OWN, rows(m), :], m, injected, pulse)
        put_field(M, (p,), m, new)

    def second_step(slot, to, s, field, g, pulse, final=False):
        p, m = 2 * s + field, 8 * g + 4
        X, z = neighbours(M, (p,), m, True)
        injected = IB[s, :, rows(8 * g), :] if field else None
        hi = N[slot, p, OWN, rows(8 * g + 8), :]
        centre = z(0)
        new = advance(field, s, centre, spread(X, z), hi, m, injected, pulse)
        if final:
            N[to, p, OWN, rows(8 * g + 8), :] = new
        else:
            put_field(N, (to, p), 8 * g + 8, new)
            if field:
                CORR[:, rows(8 * g), :] += (
                    N[slot, p - 1, OWN, rows(8 * g + 8), :] * hi
                    + M[p - 1, OWN, rows(m), :] * centre
                )

    groups = depth // 8

    def pulse_of(s, step):
        return wavelet[start_step[s] + steps - 1 - step]

    for g in range(1, groups):
        coefficients(8 * g)
    for g in range(groups):
        CORR[:, rows(8 * g), :] = zeros
    for s in range(shots):
        inject(s, 0)
        for field in range(2):
            pulse = pulse_of(s, 0)
            for g in range(1, groups):
                first_step(0, s, field, g, pulse, True)

    def arrive_first(out, inn):
        for which in range(2):
            model_copy(which, out).wait_send()
            model_copy(which, inn).wait_recv()

    def arrive_hi(p):
        def act(out, inn):
            hi_copy(p, out).wait_send()
            hi_copy(p, inn).wait_recv()

        return act

    def arrive_now(slot, p):
        def act(out, inn):
            now_copy(slot, p, out).wait_send()
            now_copy(slot, p, inn).wait_recv()

        return act

    def send_now(slot, p):
        def act(out, _):
            now_copy(slot, p, out).start()

        return act

    each_way(arrive_first)
    coefficients(0)
    coefficients(8 * groups)
    for p in range(planes):
        each_way(arrive_hi(p))

    def block(b, carry):
        slot = lax.rem(b, 2)
        to = 1 - slot
        for s in range(shots):
            pulses = [pulse_of(s, 2 * b + j) for j in range(3)]
            for field in range(2):
                p = 2 * s + field
                each_way(arrive_now(slot, p))
                for g in (0, groups):
                    first_step(slot, s, field, g, pulses[0], False)
                for g in (0, groups - 1):
                    second_step(slot, to, s, field, g, pulses[1])
                each_way(send_now(to, p))
            for field in range(2):
                for g in range(1, groups - 1):
                    second_step(slot, to, s, field, g, pulses[1])
            inject(s, b + 1)
            for field in range(2):
                for g in range(1, groups):
                    first_step(to, s, field, g, pulses[2], True)
        return carry

    lax.fori_loop(0, blocks - 1, block, 0)

    last = blocks - 1
    slot = last % 2
    to = 1 - slot
    for s in range(shots):
        for field in range(2):
            p = 2 * s + field
            each_way(arrive_now(slot, p))
            for g in (0, groups):
                first_step(slot, s, field, g, pulse_of(s, 2 * last), False)
    for g in range(groups):
        total = CORR[:, rows(8 * g), :]
        for s in range(shots):
            at = rows(8 * g + 8)
            total = total + N[slot, 2 * s, OWN, at, :] * N[slot, 2 * s + 1, OWN, at, :]
            at = rows(8 * g + 4)
            total = total + M[2 * s, OWN, at, :] * M[2 * s + 1, OWN, at, :]
        CORR[:, rows(8 * g), :] = total

    def remote(src, dst, send, recv, shot):
        return pltpu.make_async_remote_copy(
            src_ref=src,
            dst_ref=dst,
            send_sem=send,
            recv_sem=recv,
            device_id={"shot": shot},
            device_id_type=MESH,
        )

    mine = pl.ds(4 * core, 4)
    pair = remote(CORR.at[pl.ds(4 * (1 - core), 4)], PAIR, pair_send.at[0], pair_recv.at[0], partner)
    pair.start()
    for s in range(shots):
        for field in range(2):
            for g in range(groups // 2):
                second_step(slot, to, s, field, g, pulse_of(s, steps - 1), True)
    pair.wait()
    HALF[...] = CORR[mine] + PAIR[...]

    def scatter(d):
        other = lax.rem(chip + d, chips)
        return remote(
            HALF.at[:, pl.ds(other * part, part), :],
            PARTS.at[chips - d],
            rs_send.at[d],
            rs_recv.at[chips - d],
            other * 2 + core,
        )

    def scattered(d):
        return remote(HALF.at[:, pl.ds(0, part), :], PARTS.at[d], rs_send.at[d], rs_recv.at[d], partner)

    order = sorted(range(1, chips), key=lambda d: -min(d, chips - d))
    for d in order:
        scatter(d).start()
    for s in range(shots):
        for field in range(2):
            for g in range(groups // 2, groups):
                second_step(slot, to, s, field, g, pulse_of(s, steps - 1), True)

    def from_registers(get, count, slot, put):
        for r in range(8):
            T[slot, pl.ds(r, 128, stride=8), 0:count] = get(r).T
        for t in range(8):
            put(t, T[slot, 128 * t : 128 * (t + 1), 0:count].T)

    def field_out(field, ref):
        def get(r):
            return jnp.concatenate(
                [N[to, 2 * s + field, 4 + r, 8 : 8 + depth, :] for s in range(shots)], axis=0
            )

        def put(t, value):
            for s in range(shots):
                ref[s, :, 128 * t : 128 * (t + 1)] = value[depth * s : depth * (s + 1)]

        from_registers(get, shots * depth, field, put)

    field_out(0, src_out)
    for d in order:
        scattered(d).wait_recv()
    total = HALF[:, pl.ds(chip * part, part), :]
    for d in range(1, chips):
        total = total + PARTS[d]
    FIN[...] = total * (1.0 / math.sqrt(steps * shots * members))

    def gather(d):
        other = lax.rem(chip + d, chips)
        return remote(
            FIN,
            IMG.at[mine, pl.ds(chip * part, part), :],
            ag_send.at[d],
            ag_recv.at[chips - d],
            other * 2 + core,
        )

    def gathered(d):
        other = lax.rem(chip + d, chips)
        return remote(
            FIN,
            IMG.at[mine, pl.ds(other * part, part), :],
            ag_send.at[d],
            ag_recv.at[d],
            partner,
        )

    for d in order:
        gather(d).start()
    IMG[mine, pl.ds(chip * part, part), :] = FIN[...]
    field_out(1, rec_out)
    for d in order:
        gathered(d).wait_recv()
    swap = remote(IMG.at[mine], IMG.at[mine], pair_send.at[1], pair_recv.at[1], partner)
    swap.start()
    for d in range(1, chips):
        scatter(d).wait_send()
        gather(d).wait_send()
    swap.wait()

    def image_put(t, value):
        image_out[:, 128 * t : 128 * (t + 1)] = value

    from_registers(lambda r: IMG[r], depth, 0, image_put)


def local(
    courant_sq,
    sponge_level,
    source_later,
    source_now,
    receiver_later,
    receiver_now,
    traces,
    wavelet,
    source_depth,
    source_lateral,
    receiver_depth,
    receiver_lateral,
    checkpoint_step,
):
    depth, lateral = courant_sq.shape
    shots, steps, nrec = traces.shape
    members = lax.axis_size("shot")
    chips = members // 2
    part = depth // chips
    wide = depth + 8
    planes = 2 * shots
    vmem = pl.BlockSpec(memory_space=pltpu.VMEM)
    smem = pl.BlockSpec(memory_space=pltpu.SMEM)
    return pl.pallas_call(
        functools.partial(kernel, steps),
        name="rtm_window",
        out_shape=(
            jax.ShapeDtypeStruct((depth, lateral), F32),
            jax.ShapeDtypeStruct((shots, depth, lateral), F32),
            jax.ShapeDtypeStruct((shots, depth, lateral), F32),
        ),
        in_specs=[vmem] * 9 + [smem] * 4,
        out_specs=(vmem, vmem, vmem),
        scratch_shapes=[
            pltpu.VMEM((2, planes, 16, depth + 16, 128), F32),
            pltpu.VMEM((planes, 16, wide, 128), F32),
            *[pltpu.VMEM((8, wide, 128), F32) for _ in range(6)],
            pltpu.VMEM((shots, 8, wide, 128), F32),
            pltpu.VMEM((shots, 8, wide, 128), F32),
            pltpu.VMEM((shots, 8, depth, 128), F32),
            pltpu.VMEM((shots, nrec, lateral), BF16),
            pltpu.VMEM((shots, wide, nrec), F32),
            pltpu.VMEM((2, lateral, 128), F32),
            pltpu.VMEM((8, depth, 128), F32),
            pltpu.VMEM((4, depth, 128), F32),
            pltpu.VMEM((4, depth, 128), F32),
            pltpu.VMEM((chips, 4, part, 128), F32),
            pltpu.VMEM((4, part, 128), F32),
            pltpu.VMEM((8, depth, 128), F32),
            pltpu.SemaphoreType.DMA((planes, 2)),
            pltpu.SemaphoreType.DMA((2, planes, 2)),
            pltpu.SemaphoreType.DMA((planes, 2)),
            pltpu.SemaphoreType.DMA((planes, 2)),
            pltpu.SemaphoreType.DMA((2, 2)),
            pltpu.SemaphoreType.DMA((2, 2)),
            pltpu.SemaphoreType.DMA((2,)),
            pltpu.SemaphoreType.DMA((2,)),
            pltpu.SemaphoreType.DMA((chips,)),
            pltpu.SemaphoreType.DMA((chips,)),
            pltpu.SemaphoreType.DMA((chips,)),
            pltpu.SemaphoreType.DMA((chips,)),
        ],
        compiler_params=pltpu.CompilerParams(collective_id=0, has_side_effects=True),
    )(
        courant_sq,
        sponge_level,
        source_later,
        source_now,
        receiver_later,
        receiver_now,
        traces,
        receiver_depth,
        receiver_lateral,
        wavelet,
        source_depth,
        source_lateral,
        checkpoint_step,
    )


def solution(mesh):
    in_specs = (
        P(("grp", "slab"), None),
        P(("grp", "slab"), None),
        P(("grp", "shot"), "slab", None),
        P(("grp", "shot"), "slab", None),
        P(("grp", "shot"), "slab", None),
        P(("grp", "shot"), "slab", None),
        P(("grp", "shot"), None, None),
        P("grp"),
        P(("grp", "shot")),
        P(("grp", "shot")),
        P(("grp", "shot"), None),
        P(("grp", "shot"), None),
        P(("grp", "shot")),
    )
    out_specs = (
        P(("grp", "slab"), None),
        P(("grp", "shot"), "slab", None),
        P(("grp", "shot"), "slab", None),
    )
    return jax.shard_map(local, mesh=mesh, in_specs=in_specs, out_specs=out_specs, check_vma=False)
```

```python
import functools
import math

import jax
import jax.numpy as jnp
from jax import lax
from jax.experimental import pallas as pl
from jax.experimental.pallas import tpu as pltpu
from jax.sharding import PartitionSpec as P

MESH = pl.DeviceIdType.MESH
F32 = jnp.float32
BF16 = jnp.bfloat16
VMEM_LIMIT = 48 * 1024 * 1024

C0, C1, C2, C3, C4 = (-205.0 / 72.0, 8.0 / 5.0, -1.0 / 5.0, 8.0 / 315.0, -1.0 / 560.0)

OWN = slice(4, 12)


def rows(start, count=8):
    return pl.ds(start, count)


def kernel(
    steps,
    *refs,
):
    inputs, refs = refs[:13], refs[13:]
    (
        image_out,
        src_out,
        rec_out,
        courant,
        sponge,
        src_hi,
        src_now,
        rec_hi,
        rec_now,
        traces,
        rec_depth,
        rec_lateral,
        wavelet,
        src_depth,
        src_lateral,
        start_step,
        R,
        RV,
        RS,
        in_sem,
        N,
        M,
        V,
        D,
        AS,
        VS,
        AR,
        VR,
        G,
        IA,
        IB,
        W,
        DP,
        T,
        CORR,
        PAIR,
        HALF,
        PARTS,
        FIN,
        IMG,
        n_send,
        n_recv,
        h_send,
        h_recv,
        c_send,
        c_recv,
        pair_send,
        pair_recv,
        rs_send,
        rs_recv,
        ag_send,
        ag_recv,
    ) = refs
    slab, slabs = lax.axis_index("slab"), lax.axis_size("slab")
    me, members = lax.axis_index("shot"), lax.axis_size("shot")
    chips = members // 2
    chip, core = me // 2, lax.rem(me, 2)
    depth = courant.shape[0]
    shots = src_now.shape[0]
    nrec = traces.shape[2]
    blocks = steps // 2
    wide = depth + 8
    first = slab * depth
    has_up, has_down = slab > 0, slab < slabs - 1
    part = depth // chips
    planes = 2 * shots

    barrier = pltpu.get_barrier_semaphore()

    def greet(target):
        pl.semaphore_signal(barrier, inc=1, device_id=target, device_id_type=MESH)

    @pl.when(has_up)
    def _():
        greet({"slab": slab - 1})

    @pl.when(has_down)
    def _():
        greet({"slab": slab + 1})

    partner = chip * 2 + (1 - core)
    greet({"shot": partner})
    peers = [lax.rem(chip + d, chips) * 2 + core for d in range(1, chips)]
    for peer in peers:
        greet({"shot": peer})

    local_refs = (
        courant, sponge, src_hi, src_now, rec_hi, rec_now, traces, rec_depth, rec_lateral,
        wavelet, src_depth, src_lateral, start_step,
    )
    loads = [
        pltpu.make_async_copy(inputs[i], local_refs[i], in_sem.at[i])
        for i in (3, 2, 5, 4, 0, 1, 6, 7, 8, 9, 10, 11, 12)
    ]
    for load in loads:
        load.start()

    lane = lax.broadcasted_iota(jnp.int32, (4, 8, 128), 2)
    lane8 = lax.broadcasted_iota(jnp.int32, (8, 8, 128), 2)
    reg8 = lax.broadcasted_iota(jnp.int32, (8, 8, 128), 0)
    row8 = lax.broadcasted_iota(jnp.int32, (8, 8, 128), 1)
    cell8 = 8 * lane8 + reg8

    def up_lane(v):
        return jnp.where(lane == 0, 0.0, pltpu.roll(v, 1, axis=2))

    def down_lane(v):
        return jnp.where(lane == 127, 0.0, pltpu.roll(v, 127, axis=2))

    def to_registers(block, count, slot, put):
        for t in range(8):
            T[slot, 128 * t : 128 * (t + 1), 0:count] = block(t).T
        for r in range(8):
            put(r, T[slot, pl.ds(r, 128, stride=8), 0:count].T)

    def field_block(ref):
        return lambda t: ref[:, :, 128 * t : 128 * (t + 1)].reshape(shots * depth, 128)

    def put_now(field):
        def put(r, value):
            for s in range(shots):
                v = value[depth * s : depth * (s + 1)]
                N[0, 2 * s + field, 4 + r, 8 : 8 + depth, :] = v
                edge = lax.broadcasted_iota(jnp.int32, (depth, 128), 1)
                if r < 4:
                    N[0, 2 * s + field, 12 + r, 8 : 8 + depth, :] = jnp.where(
                        edge == 127, 0.0, pltpu.roll(v, 127, axis=1)
                    )
                else:
                    N[0, 2 * s + field, r - 4, 8 : 8 + depth, :] = jnp.where(
                        edge == 0, 0.0, pltpu.roll(v, 1, axis=1)
                    )

        return put

    def put_hi(field):
        def put(r, value):
            for s in range(shots):
                M[2 * s + field, 4 + r, 4 : 4 + depth, :] = value[depth * s : depth * (s + 1)]

        return put

    def model_block(t):
        cols = slice(128 * t, 128 * (t + 1))
        return jnp.concatenate(
            [courant[:, cols], 1.0 - 0.06 * sponge[:, cols].astype(F32)], axis=0
        )

    def put_model(r, value):
        V[r, 4 : 4 + depth, :] = value[:depth]
        D[r, 4 : 4 + depth, :] = value[depth:]

    zeros = jnp.zeros((8, 8, 128), F32)

    def clear(side):
        for p in range(planes):
            R[p, 16 * side : 16 * (side + 1), :] = jnp.zeros((16, 1024), F32)
            for slot in range(2):
                N[slot, p, OWN, rows((8 + depth) * side), :] = zeros
        RV[8 * side : 8 * (side + 1), :] = jnp.zeros((8, 1024), F32)
        RS[8 * side : 8 * (side + 1), :] = jnp.zeros((8, 1024), jnp.int32)

    @pl.when(slab == 0)
    def _():
        clear(0)

    @pl.when(slab == slabs - 1)
    def _():
        clear(1)

    def shift(ref_at, src_row, dst_row, count, send, recv, to):
        return pltpu.make_async_remote_copy(
            src_ref=ref_at(src_row, count),
            dst_ref=ref_at(dst_row, count),
            send_sem=send,
            recv_sem=recv,
            device_id={"slab": to},
            device_id_type=MESH,
        )

    def now_copy(slot, p, direction):
        at = lambda row, count: N.at[slot, p, OWN, pl.ds(row, count), :]
        if direction == 0:
            return shift(at, 8, 8 + depth, 8, n_send.at[p, 0], n_recv.at[slot, p, 0], slab - 1)
        return shift(at, depth, 0, 8, n_send.at[p, 1], n_recv.at[slot, p, 1], slab + 1)

    fields = (src_now, src_hi), (rec_now, rec_hi)

    def raw(src, dst, send, recv, direction):
        return pltpu.make_async_remote_copy(
            src_ref=src,
            dst_ref=dst,
            send_sem=send,
            recv_sem=recv,
            device_id={"slab": slab - 1 if direction == 0 else slab + 1},
            device_id_type=MESH,
        )

    def raw_now(p, direction):
        row = 0 if direction == 0 else depth - 8
        return raw(
            fields[p % 2][0].at[p // 2, pl.ds(row, 8), :],
            R.at[p, pl.ds(16 * (1 - direction), 8), :],
            n_send.at[p, direction],
            n_recv.at[0, p, direction],
            direction,
        )

    def raw_hi(p, direction):
        row = 0 if direction == 0 else depth - 4
        return raw(
            fields[p % 2][1].at[p // 2, pl.ds(row, 4), :],
            R.at[p, pl.ds(16 * (1 - direction) + 8, 4), :],
            h_send.at[p, direction],
            h_recv.at[p, direction],
            direction,
        )

    def raw_model(which, direction):
        row = 0 if direction == 0 else depth - 4
        return raw(
            (courant, sponge)[which].at[pl.ds(row, 4), :],
            (RV, RS)[which].at[pl.ds(8 * (1 - direction), 4), :],
            c_send.at[which, direction],
            c_recv.at[which, direction],
            direction,
        )

    def each_way(act):
        @pl.when(has_up)
        def _():
            act(0, 1)

        @pl.when(has_down)
        def _():
            act(1, 0)

    greeted = (
        has_up.astype(jnp.int32) + has_down.astype(jnp.int32) + len(peers) + 1
    )
    pl.semaphore_wait(barrier, greeted)

    for load in loads[:6]:
        load.wait()

    def send_first(out, _):
        raw_model(0, out).start()
        raw_model(1, out).start()
        for p in range(planes):
            raw_now(p, out).start()
            raw_hi(p, out).start()

    each_way(send_first)

    to_registers(model_block, shots * depth, 0, put_model)
    for field in range(2):
        to_registers(field_block(fields[field][0]), shots * depth, 1, put_now(field))
        to_registers(field_block(fields[field][1]), shots * depth, 0, put_hi(field))
    for load in loads[6:]:
        load.wait()

    pad = 16 * ((wide + 15) // 16)
    top = 2 * pad

    rec_ids = first - 4 + lax.broadcasted_iota(jnp.int32, (wide, nrec), 0)
    for s in range(shots):
        DP[s] = (rec_ids == rec_depth[s : s + 1, :]).astype(F32)
        for q in range(nrec // 128):
            wanted = jnp.broadcast_to(
                rec_lateral[s : s + 1, 128 * q : 128 * (q + 1)].astype(F32), (128, 128)
            ).T
            at = lax.broadcasted_iota(jnp.int32, (128, 128), 1).astype(F32) * 8.0
            for r in range(8):
                W[s, 128 * q : 128 * (q + 1), 128 * r : 128 * (r + 1)] = (
                    (wanted == at + float(r)).astype(F32).astype(BF16)
                )

    span = 2 * (pad + depth)

    def inject(s, block):
        def terms(step):
            t = traces[s, pl.ds(step, 1), :] * (1.0 / C1)
            hi = t.astype(BF16).astype(F32)
            return hi, t - hi

        gap = jnp.zeros((pad - wide, nrec), F32)
        table = []
        for e in range(2):
            for term in terms(2 * (block + e)):
                table += [DP[s] * term, gap]
            for term in terms(2 * (block + e) + 1):
                table += [DP[s, 4 : 4 + depth, :] * term]
        table = jnp.concatenate(table, axis=0).astype(BF16)
        for c in range(4):
            both = jnp.dot(
                table, W[s, :, 256 * c : 256 * (c + 1)], preferred_element_type=F32
            )
            for e in range(2):
                got = both[span * e : span * (e + 1)]
                a = got[0:wide] + got[pad : pad + wide]
                b = got[top : top + depth] + got[top + depth : top + 2 * depth]
                for h in range(2):
                    IA[s, block + e, 2 * c + h] = a[:, 128 * h : 128 * (h + 1)]
                    IB[s, block + e, 2 * c + h] = b[:, 128 * h : 128 * (h + 1)]

    def coefficients(m):
        at = rows(m)
        v, d = V[:, at, :], D[:, at, :]
        a = 2.0 + (2.0 * C0) * v
        AS[:, at, :] = a
        AR[:, at, :] = d * a
        VS[:, at, :] = C1 * v
        VR[:, at, :] = (C1 * d) * v
        for s in range(shots):
            hit = (cell8 == src_lateral[s]) & (row8 + (first - 4 + m) == src_depth[s])
            G[s, :, at, :] = jnp.where(hit, -v, 0.0)

    def spread(X, z):
        total = None
        for k, a in ((1, None), (2, C2 / C1), (3, C3 / C1), (4, C4 / C1)):
            pair = (X(4 + k) + X(4 - k)) + (z(k) + z(-k))
            total = pair if a is None else total + a * pair
        return total

    def neighbours(ref, pre, row, stored):
        z = lambda k: ref[pre + (OWN, rows(row + k), slice(None))]
        if stored:
            X = lambda k: ref[pre + (slice(k, k + 8), rows(row), slice(None))]
            return X, z
        c = z(0)
        wide_c = jnp.concatenate([up_lane(c[4:]), c, down_lane(c[:4])], axis=0)
        return (lambda k: wide_c[k : k + 8]), z

    def advance(field, s, centre, total, hi, m, injected, pulse):
        at = rows(m)
        if field == 0:
            return AS[:, at, :] * centre - hi + (VS[:, at, :] * total + pulse * G[s, :, at, :])
        return AR[:, at, :] * centre - D[:, at, :] * hi + VR[:, at, :] * (total + injected)

    def put_field(ref, pre, row, value):
        at = rows(row)
        ref[pre + (OWN, at, slice(None))] = value
        ref[pre + (slice(12, 16), at, slice(None))] = down_lane(value[:4])
        ref[pre + (slice(0, 4), at, slice(None))] = up_lane(value[4:])

    def first_step(slot, b, s, field, g, pulse, stored):
        p, m = 2 * s + field, 8 * g
        X, z = neighbours(N, (slot, p), m + 4, stored)
        injected = IA[s, b, :, rows(m), :] if field else None
        new = advance(field, s, z(0), spread(X, z), M[p, OWN, rows(m), :], m, injected, pulse)
        put_field(M, (p,), m, new)

    def second_step(slot, to, b, s, field, g, pulse, final=False):
        p, m = 2 * s + field, 8 * g + 4
        X, z = neighbours(M, (p,), m, True)
        injected = IB[s, b, :, rows(8 * g), :] if field else None
        hi = N[slot, p, OWN, rows(8 * g + 8), :]
        centre = z(0)
        new = advance(field, s, centre, spread(X, z), hi, m, injected, pulse)
        if final:
            N[to, p, OWN, rows(8 * g + 8), :] = new
        else:
            put_field(N, (to, p), 8 * g + 8, new)
            if field:
                CORR[:, rows(8 * g), :] += (
                    N[slot, p - 1, OWN, rows(8 * g + 8), :] * hi
                    + M[p - 1, OWN, rows(m), :] * centre
                )

    groups = depth // 8

    def pulse_of(s, step):
        return wavelet[start_step[s] + steps - 1 - step]

    for g in range(1, groups):
        coefficients(8 * g)
    for g in range(groups):
        CORR[:, rows(8 * g), :] = zeros
    for s in range(shots):
        inject(s, 0)
        for field in range(2):
            pulse = pulse_of(s, 0)
            for g in range(1, groups):
                first_step(0, 0, s, field, g, pulse, True)

    def later_blocks(i, carry):
        for s in range(shots):
            inject(s, 2 * i)
        return carry

    lax.fori_loop(1, blocks // 2, later_blocks, 0)

    def arrive_now(slot, p):
        def act(out, inn):
            now_copy(slot, p, out).wait_send()
            now_copy(slot, p, inn).wait_recv()

        return act

    def send_now(slot, p):
        def act(out, _):
            now_copy(slot, p, out).start()

        return act

    def arrive_raw(copies):
        def act(out, inn):
            for copy in copies:
                copy(out).wait_send()
                copy(inn).wait_recv()

        return act

    each_way(arrive_raw([functools.partial(raw_model, 0), functools.partial(raw_model, 1)]))

    def edge_model(t):
        cols = slice(128 * t, 128 * (t + 1))
        return jnp.concatenate([RV[:, cols], 1.0 - 0.06 * RS[:, cols].astype(F32)], axis=0)

    def put_edge_model(r, value):
        V[r, 0:4, :] = value[0:4]
        V[r, 4 + depth : 8 + depth, :] = value[8:12]
        D[r, 0:4, :] = value[16:20]
        D[r, 4 + depth : 8 + depth, :] = value[24:28]

    to_registers(edge_model, 32, 0, put_edge_model)
    coefficients(0)
    coefficients(8 * groups)

    def edge_rows(p):
        def put(r, value):
            N[0, p, 4 + r, 0:8, :] = value[0:8]
            M[p, 4 + r, 0:4, :] = value[8:12]
            N[0, p, 4 + r, 8 + depth : 16 + depth, :] = value[16:24]
            M[p, 4 + r, 4 + depth : 8 + depth, :] = value[24:28]

        to_registers(lambda t: R[p, :, 128 * t : 128 * (t + 1)], 32, (p + 1) % 2, put)

    for p in range(planes):
        each_way(arrive_raw([functools.partial(raw_now, p), functools.partial(raw_hi, p)]))
        edge_rows(p)
        for g in (0, groups):
            first_step(0, 0, p // 2, p % 2, g, pulse_of(p // 2, 0), False)
        for g in (0, groups - 1):
            second_step(0, 1, 0, p // 2, p % 2, g, pulse_of(p // 2, 1))
        each_way(send_now(1, p))

    def edges(b, slot, to, s, field, pulses):
        p = 2 * s + field
        each_way(arrive_now(slot, p))
        for g in (0, groups):
            first_step(slot, b, s, field, g, pulses[0], False)
        for g in (0, groups - 1):
            second_step(slot, to, b, s, field, g, pulses[1])
        each_way(send_now(to, p))

    def inner(b, slot, to, s, pulses):
        for field in range(2):
            for g in range(1, groups - 1):
                second_step(slot, to, b, s, field, g, pulses[1])
        for field in range(2):
            for g in range(1, groups):
                first_step(to, b + 1, s, field, g, pulses[2], True)

    def pulses_of(s, b):
        return [pulse_of(s, 2 * b + j) for j in range(3)]

    for s in range(shots):
        inner(0, 0, 1, s, pulses_of(s, 0))

    def block(b, carry):
        slot = lax.rem(b, 2)
        to = 1 - slot
        for s in range(shots):
            pulses = pulses_of(s, b)
            for field in range(2):
                edges(b, slot, to, s, field, pulses)
            inner(b, slot, to, s, pulses)
        return carry

    lax.fori_loop(1, blocks - 1, block, 0)

    last = blocks - 1
    slot = last % 2
    to = 1 - slot
    for s in range(shots):
        for field in range(2):
            p = 2 * s + field
            each_way(arrive_now(slot, p))
            for g in (0, groups):
                first_step(slot, last, s, field, g, pulse_of(s, 2 * last), False)
    for g in range(groups):
        total = CORR[:, rows(8 * g), :]
        for s in range(shots):
            at = rows(8 * g + 8)
            total = total + N[slot, 2 * s, OWN, at, :] * N[slot, 2 * s + 1, OWN, at, :]
            at = rows(8 * g + 4)
            total = total + M[2 * s, OWN, at, :] * M[2 * s + 1, OWN, at, :]
        CORR[:, rows(8 * g), :] = total

    def remote(src, dst, send, recv, shot):
        return pltpu.make_async_remote_copy(
            src_ref=src,
            dst_ref=dst,
            send_sem=send,
            recv_sem=recv,
            device_id={"shot": shot},
            device_id_type=MESH,
        )

    mine = pl.ds(4 * core, 4)
    pair = remote(CORR.at[pl.ds(4 * (1 - core), 4)], PAIR, pair_send.at[0], pair_recv.at[0], partner)
    pair.start()
    for s in range(shots):
        for field in range(2):
            for g in range(groups // 2):
                second_step(slot, to, last, s, field, g, pulse_of(s, steps - 1), True)
    pair.wait()
    HALF[...] = CORR[mine] + PAIR[...]

    def scatter(d):
        other = lax.rem(chip + d, chips)
        return remote(
            HALF.at[:, pl.ds(other * part, part), :],
            PARTS.at[chips - d],
            rs_send.at[d],
            rs_recv.at[chips - d],
            other * 2 + core,
        )

    def scattered(d):
        return remote(HALF.at[:, pl.ds(0, part), :], PARTS.at[d], rs_send.at[d], rs_recv.at[d], partner)

    order = sorted(range(1, chips), key=lambda d: -min(d, chips - d))
    for d in order:
        scatter(d).start()
    for s in range(shots):
        for field in range(2):
            for g in range(groups // 2, groups):
                second_step(slot, to, last, s, field, g, pulse_of(s, steps - 1), True)

    def from_registers(get, count, slot, put):
        for r in range(8):
            T[slot, pl.ds(r, 128, stride=8), 0:count] = get(r).T
        for t in range(8):
            put(t, T[slot, 128 * t : 128 * (t + 1), 0:count].T)

    def field_out(field, ref):
        def get(r):
            return jnp.concatenate(
                [N[to, 2 * s + field, 4 + r, 8 : 8 + depth, :] for s in range(shots)], axis=0
            )

        def put(t, value):
            for s in range(shots):
                ref[s, :, 128 * t : 128 * (t + 1)] = value[depth * s : depth * (s + 1)]

        from_registers(get, shots * depth, field, put)

    field_out(0, src_out)
    for d in order:
        scattered(d).wait_recv()
    total = HALF[:, pl.ds(chip * part, part), :]
    for d in range(1, chips):
        total = total + PARTS[d]
    FIN[...] = total * (1.0 / math.sqrt(steps * shots * members))

    def gather(d):
        other = lax.rem(chip + d, chips)
        return remote(
            FIN,
            IMG.at[mine, pl.ds(chip * part, part), :],
            ag_send.at[d],
            ag_recv.at[chips - d],
            other * 2 + core,
        )

    def gathered(d):
        other = lax.rem(chip + d, chips)
        return remote(
            FIN,
            IMG.at[mine, pl.ds(other * part, part), :],
            ag_send.at[d],
            ag_recv.at[d],
            partner,
        )

    for d in order:
        gather(d).start()
    IMG[mine, pl.ds(chip * part, part), :] = FIN[...]
    field_out(1, rec_out)
    for d in order:
        gathered(d).wait_recv()
    swap = remote(IMG.at[mine], IMG.at[mine], pair_send.at[1], pair_recv.at[1], partner)
    swap.start()
    for d in range(1, chips):
        scatter(d).wait_send()
        gather(d).wait_send()
    swap.wait()

    image_out[...] = IMG[...]


def finish(image, src, rec, image_out, src_out, rec_out, T, natural, sem):
    copies = [
        pltpu.make_async_copy(src, src_out, sem.at[1]),
        pltpu.make_async_copy(rec, rec_out, sem.at[2]),
    ]
    for copy in copies:
        copy.start()
    depth = image.shape[1]
    for r in range(8):
        T[pl.ds(r, 128, stride=8), 0:depth] = image[r].T
    for t in range(8):
        natural[:, 128 * t : 128 * (t + 1)] = T[128 * t : 128 * (t + 1), 0:depth].T
    copies.append(pltpu.make_async_copy(natural, image_out, sem.at[0]))
    copies[-1].start()
    for copy in copies:
        copy.wait()


def local(
    courant_sq,
    sponge_level,
    source_later,
    source_now,
    receiver_later,
    receiver_now,
    traces,
    wavelet,
    source_depth,
    source_lateral,
    receiver_depth,
    receiver_lateral,
    checkpoint_step,
):
    depth, lateral = courant_sq.shape
    shots, steps, nrec = traces.shape
    members = lax.axis_size("shot")
    chips = members // 2
    part = depth // chips
    wide = depth + 8
    planes = 2 * shots
    vmem = pl.BlockSpec(memory_space=pltpu.VMEM)
    image, src_out, rec_out = pl.pallas_call(
        functools.partial(kernel, steps),
        name="rtm_window",
        out_shape=(
            jax.ShapeDtypeStruct((8, depth, 128), F32),
            jax.ShapeDtypeStruct((shots, depth, lateral), F32),
            jax.ShapeDtypeStruct((shots, depth, lateral), F32),
        ),
        in_specs=[pl.BlockSpec(memory_space=pltpu.HBM)] * 13,
        out_specs=(vmem, vmem, vmem),
        scratch_shapes=[
            pltpu.VMEM((depth, lateral), F32),
            pltpu.VMEM((depth, lateral), jnp.int32),
            *[pltpu.VMEM((shots, depth, lateral), F32) for _ in range(4)],
            pltpu.VMEM(traces.shape, F32),
            pltpu.VMEM(receiver_depth.shape, jnp.int32),
            pltpu.VMEM(receiver_lateral.shape, jnp.int32),
            pltpu.SMEM(wavelet.shape, F32),
            pltpu.SMEM(source_depth.shape, jnp.int32),
            pltpu.SMEM(source_lateral.shape, jnp.int32),
            pltpu.SMEM(checkpoint_step.shape, jnp.int32),
            pltpu.VMEM((planes, 32, lateral), F32),
            pltpu.VMEM((16, lateral), F32),
            pltpu.VMEM((16, lateral), jnp.int32),
            pltpu.SemaphoreType.DMA((13,)),
            pltpu.VMEM((2, planes, 16, depth + 16, 128), F32),
            pltpu.VMEM((planes, 16, wide, 128), F32),
            *[pltpu.VMEM((8, wide, 128), F32) for _ in range(6)],
            pltpu.VMEM((shots, 8, wide, 128), F32),
            pltpu.VMEM((shots, steps // 2, 8, wide, 128), F32),
            pltpu.VMEM((shots, steps // 2, 8, depth, 128), F32),
            pltpu.VMEM((shots, nrec, lateral), BF16),
            pltpu.VMEM((shots, wide, nrec), F32),
            pltpu.VMEM((2, lateral, 128), F32),
            pltpu.VMEM((8, depth, 128), F32),
            pltpu.VMEM((4, depth, 128), F32),
            pltpu.VMEM((4, depth, 128), F32),
            pltpu.VMEM((chips, 4, part, 128), F32),
            pltpu.VMEM((4, part, 128), F32),
            pltpu.VMEM((8, depth, 128), F32),
            pltpu.SemaphoreType.DMA((planes, 2)),
            pltpu.SemaphoreType.DMA((2, planes, 2)),
            pltpu.SemaphoreType.DMA((planes, 2)),
            pltpu.SemaphoreType.DMA((planes, 2)),
            pltpu.SemaphoreType.DMA((2, 2)),
            pltpu.SemaphoreType.DMA((2, 2)),
            pltpu.SemaphoreType.DMA((2,)),
            pltpu.SemaphoreType.DMA((2,)),
            pltpu.SemaphoreType.DMA((chips,)),
            pltpu.SemaphoreType.DMA((chips,)),
            pltpu.SemaphoreType.DMA((chips,)),
            pltpu.SemaphoreType.DMA((chips,)),
        ],
        compiler_params=pltpu.CompilerParams(
            collective_id=0, has_side_effects=True, vmem_limit_bytes=VMEM_LIMIT
        ),
    )(
        *[
            pltpu.with_memory_space_constraint(x, pltpu.HBM)
            for x in (
                courant_sq,
                sponge_level,
                source_later,
                source_now,
                receiver_later,
                receiver_now,
                traces,
                receiver_depth,
                receiver_lateral,
                wavelet,
                source_depth,
                source_lateral,
                checkpoint_step,
            )
        ]
    )
    return pl.pallas_call(
        finish,
        name="finish",
        out_shape=(
            jax.ShapeDtypeStruct((depth, lateral), F32),
            jax.ShapeDtypeStruct((shots, depth, lateral), F32),
            jax.ShapeDtypeStruct((shots, depth, lateral), F32),
        ),
        in_specs=[vmem] * 3,
        out_specs=(pl.BlockSpec(memory_space=pltpu.HBM),) * 3,
        scratch_shapes=[
            pltpu.VMEM((lateral, 128), F32),
            pltpu.VMEM((depth, lateral), F32),
            pltpu.SemaphoreType.DMA((3,)),
        ],
        compiler_params=pltpu.CompilerParams(vmem_limit_bytes=VMEM_LIMIT),
    )(image, src_out, rec_out)


def solution(mesh):
    in_specs = (
        P(("grp", "slab"), None),
        P(("grp", "slab"), None),
        P(("grp", "shot"), "slab", None),
        P(("grp", "shot"), "slab", None),
        P(("grp", "shot"), "slab", None),
        P(("grp", "shot"), "slab", None),
        P(("grp", "shot"), None, None),
        P("grp"),
        P(("grp", "shot")),
        P(("grp", "shot")),
        P(("grp", "shot"), None),
        P(("grp", "shot"), None),
        P(("grp", "shot")),
    )
    out_specs = (
        P(("grp", "slab"), None),
        P(("grp", "shot"), "slab", None),
        P(("grp", "shot"), "slab", None),
    )
    return jax.shard_map(local, mesh=mesh, in_specs=in_specs, out_specs=out_specs, check_vma=False)
```

```python
import functools
import math

import jax
import jax.numpy as jnp
from jax import lax
from jax.experimental import pallas as pl
from jax.experimental.pallas import tpu as pltpu
from jax.sharding import PartitionSpec as P

MESH = pl.DeviceIdType.MESH
F32 = jnp.float32
BF16 = jnp.bfloat16
VMEM_LIMIT = 48 * 1024 * 1024

C0, C1, C2, C3, C4 = (-205.0 / 72.0, 8.0 / 5.0, -1.0 / 5.0, 8.0 / 315.0, -1.0 / 560.0)

OWN = slice(4, 12)


def rows(start, count=8):
    return pl.ds(start, count)


def kernel(
    steps,
    *refs,
):
    inputs, refs = refs[:13], refs[13:]
    (
        image_out,
        src_out,
        rec_out,
        courant,
        sponge,
        src_hi,
        src_now,
        rec_hi,
        rec_now,
        traces,
        rec_depth,
        rec_lateral,
        wavelet,
        src_depth,
        src_lateral,
        start_step,
        R,
        RV,
        RS,
        in_sem,
        N,
        M,
        V,
        D,
        AS,
        VS,
        AR,
        VR,
        G,
        IA,
        IB,
        W,
        DP,
        T,
        CORR,
        PAIR,
        HALF,
        PARTS,
        FIN,
        IMG,
        LATE,
        LPAIR,
        LHALF,
        LPARTS,
        LSUM,
        n_send,
        n_recv,
        h_send,
        h_recv,
        c_send,
        c_recv,
        pair_send,
        pair_recv,
        rs_send,
        rs_recv,
        ag_send,
        ag_recv,
        l_send,
        l_recv,
    ) = refs
    slab, slabs = lax.axis_index("slab"), lax.axis_size("slab")
    me, members = lax.axis_index("shot"), lax.axis_size("shot")
    chips = members // 2
    chip, core = me // 2, lax.rem(me, 2)
    depth = courant.shape[0]
    shots = src_now.shape[0]
    nrec = traces.shape[2]
    blocks = steps // 2
    wide = depth + 8
    first = slab * depth
    has_up, has_down = slab > 0, slab < slabs - 1
    part = depth // chips
    planes = 2 * shots

    barrier = pltpu.get_barrier_semaphore()

    def greet(target):
        pl.semaphore_signal(barrier, inc=1, device_id=target, device_id_type=MESH)

    @pl.when(has_up)
    def _():
        greet({"slab": slab - 1})

    @pl.when(has_down)
    def _():
        greet({"slab": slab + 1})

    partner = chip * 2 + (1 - core)
    greet({"shot": partner})
    peers = [lax.rem(chip + d, chips) * 2 + core for d in range(1, chips)]
    for peer in peers:
        greet({"shot": peer})

    local_refs = (
        courant, sponge, src_hi, src_now, rec_hi, rec_now, traces, rec_depth, rec_lateral,
        wavelet, src_depth, src_lateral, start_step,
    )
    loads = [
        pltpu.make_async_copy(inputs[i], local_refs[i], in_sem.at[i])
        for i in (0, 1, 3, 2, 5, 4, 9, 10, 11, 12, 6, 7, 8)
    ]
    for load in loads:
        load.start()

    lane = lax.broadcasted_iota(jnp.int32, (4, 8, 128), 2)
    lane8 = lax.broadcasted_iota(jnp.int32, (8, 8, 128), 2)
    reg8 = lax.broadcasted_iota(jnp.int32, (8, 8, 128), 0)
    row8 = lax.broadcasted_iota(jnp.int32, (8, 8, 128), 1)
    cell8 = 8 * lane8 + reg8

    def up_lane(v):
        return jnp.where(lane == 0, 0.0, pltpu.roll(v, 1, axis=2))

    def down_lane(v):
        return jnp.where(lane == 127, 0.0, pltpu.roll(v, 127, axis=2))

    def to_registers(block, count, slot, put):
        for t in range(8):
            T[slot, 128 * t : 128 * (t + 1), 0:count] = block(t).T
        for r in range(8):
            put(r, T[slot, pl.ds(r, 128, stride=8), 0:count].T)

    def field_block(ref):
        return lambda t: ref[:, :, 128 * t : 128 * (t + 1)].reshape(shots * depth, 128)

    def put_now(field):
        def put(r, value):
            for s in range(shots):
                v = value[depth * s : depth * (s + 1)]
                N[0, 2 * s + field, 4 + r, 8 : 8 + depth, :] = v
                edge = lax.broadcasted_iota(jnp.int32, (depth, 128), 1)
                if r < 4:
                    N[0, 2 * s + field, 12 + r, 8 : 8 + depth, :] = jnp.where(
                        edge == 127, 0.0, pltpu.roll(v, 127, axis=1)
                    )
                else:
                    N[0, 2 * s + field, r - 4, 8 : 8 + depth, :] = jnp.where(
                        edge == 0, 0.0, pltpu.roll(v, 1, axis=1)
                    )

        return put

    def put_hi(field):
        def put(r, value):
            for s in range(shots):
                M[2 * s + field, 4 + r, 4 : 4 + depth, :] = value[depth * s : depth * (s + 1)]

        return put

    def model_block(t):
        cols = slice(128 * t, 128 * (t + 1))
        return jnp.concatenate(
            [courant[:, cols], 1.0 - 0.06 * sponge[:, cols].astype(F32)], axis=0
        )

    def put_model(r, value):
        V[r, 4 : 4 + depth, :] = value[:depth]
        D[r, 4 : 4 + depth, :] = value[depth:]

    zeros = jnp.zeros((8, 8, 128), F32)

    def clear(side):
        for p in range(planes):
            R[p, 16 * side : 16 * (side + 1), :] = jnp.zeros((16, 1024), F32)
            for slot in range(2):
                N[slot, p, OWN, rows((8 + depth) * side), :] = zeros
        RV[8 * side : 8 * (side + 1), :] = jnp.zeros((8, 1024), F32)
        RS[8 * side : 8 * (side + 1), :] = jnp.zeros((8, 1024), jnp.int32)

    @pl.when(slab == 0)
    def _():
        clear(0)

    @pl.when(slab == slabs - 1)
    def _():
        clear(1)

    def shift(ref_at, src_row, dst_row, count, send, recv, to):
        return pltpu.make_async_remote_copy(
            src_ref=ref_at(src_row, count),
            dst_ref=ref_at(dst_row, count),
            send_sem=send,
            recv_sem=recv,
            device_id={"slab": to},
            device_id_type=MESH,
        )

    def now_copy(slot, p, direction):
        at = lambda row, count: N.at[slot, p, OWN, pl.ds(row, count), :]
        if direction == 0:
            return shift(at, 8, 8 + depth, 8, n_send.at[p, 0], n_recv.at[slot, p, 0], slab - 1)
        return shift(at, depth, 0, 8, n_send.at[p, 1], n_recv.at[slot, p, 1], slab + 1)

    fields = (src_now, src_hi), (rec_now, rec_hi)

    def raw(src, dst, send, recv, direction):
        return pltpu.make_async_remote_copy(
            src_ref=src,
            dst_ref=dst,
            send_sem=send,
            recv_sem=recv,
            device_id={"slab": slab - 1 if direction == 0 else slab + 1},
            device_id_type=MESH,
        )

    def raw_now(p, direction):
        row = 0 if direction == 0 else depth - 8
        return raw(
            fields[p % 2][0].at[p // 2, pl.ds(row, 8), :],
            R.at[p, pl.ds(16 * (1 - direction), 8), :],
            n_send.at[p, direction],
            n_recv.at[0, p, direction],
            direction,
        )

    def raw_hi(p, direction):
        row = 0 if direction == 0 else depth - 4
        return raw(
            fields[p % 2][1].at[p // 2, pl.ds(row, 4), :],
            R.at[p, pl.ds(16 * (1 - direction) + 8, 4), :],
            h_send.at[p, direction],
            h_recv.at[p, direction],
            direction,
        )

    def raw_model(which, direction):
        row = 0 if direction == 0 else depth - 4
        return raw(
            (courant, sponge)[which].at[pl.ds(row, 4), :],
            (RV, RS)[which].at[pl.ds(8 * (1 - direction), 4), :],
            c_send.at[which, direction],
            c_recv.at[which, direction],
            direction,
        )

    def each_way(act):
        @pl.when(has_up)
        def _():
            act(0, 1)

        @pl.when(has_down)
        def _():
            act(1, 0)

    greeted = (
        has_up.astype(jnp.int32) + has_down.astype(jnp.int32) + len(peers) + 1
    )
    pl.semaphore_wait(barrier, greeted)

    for load in loads[:6]:
        load.wait()

    def send_first(out, _):
        raw_model(0, out).start()
        raw_model(1, out).start()
        for field in range(2):
            for s in range(shots):
                raw_now(2 * s + field, out).start()
                raw_hi(2 * s + field, out).start()

    each_way(send_first)

    def field_in(field):
        to_registers(field_block(fields[field][0]), shots * depth, 1, put_now(field))
        to_registers(field_block(fields[field][1]), shots * depth, 0, put_hi(field))

    to_registers(model_block, shots * depth, 0, put_model)
    field_in(0)
    for load in loads[6:]:
        load.wait()

    pad = 16 * ((wide + 15) // 16)
    top = 2 * pad

    def tables():
        rec_ids = first - 4 + lax.broadcasted_iota(jnp.int32, (wide, nrec), 0)
        for s in range(shots):
            DP[s] = (rec_ids == rec_depth[s : s + 1, :]).astype(F32)
            for q in range(nrec // 128):
                wanted = jnp.broadcast_to(
                    rec_lateral[s : s + 1, 128 * q : 128 * (q + 1)].astype(F32), (128, 128)
                ).T
                at = lax.broadcasted_iota(jnp.int32, (128, 128), 1).astype(F32) * 8.0
                for r in range(8):
                    W[s, 128 * q : 128 * (q + 1), 128 * r : 128 * (r + 1)] = (
                        (wanted == at + float(r)).astype(F32).astype(BF16)
                    )

    span = 2 * (pad + depth)

    def inject(s, block):
        def terms(step):
            t = traces[s, pl.ds(step, 1), :] * (1.0 / C1)
            hi = t.astype(BF16).astype(F32)
            return hi, t - hi

        gap = jnp.zeros((pad - wide, nrec), F32)
        table = []
        for e in range(2):
            for term in terms(2 * (block + e)):
                table += [DP[s] * term, gap]
            for term in terms(2 * (block + e) + 1):
                table += [DP[s, 4 : 4 + depth, :] * term]
        table = jnp.concatenate(table, axis=0).astype(BF16)
        for c in range(4):
            both = jnp.dot(
                table, W[s, :, 256 * c : 256 * (c + 1)], preferred_element_type=F32
            )
            for e in range(2):
                got = both[span * e : span * (e + 1)]
                a = got[0:wide] + got[pad : pad + wide]
                b = got[top : top + depth] + got[top + depth : top + 2 * depth]
                for h in range(2):
                    IA[s, block + e, 2 * c + h] = a[:, 128 * h : 128 * (h + 1)]
                    IB[s, block + e, 2 * c + h] = b[:, 128 * h : 128 * (h + 1)]

    def coefficients(m):
        at = rows(m)
        v, d = V[:, at, :], D[:, at, :]
        a = 2.0 + (2.0 * C0) * v
        AS[:, at, :] = a
        AR[:, at, :] = d * a
        VS[:, at, :] = C1 * v
        VR[:, at, :] = (C1 * d) * v
        for s in range(shots):
            hit = (cell8 == src_lateral[s]) & (row8 + (first - 4 + m) == src_depth[s])
            G[s, :, at, :] = jnp.where(hit, -v, 0.0)

    def spread(X, z):
        total = None
        for k, a in ((1, None), (2, C2 / C1), (3, C3 / C1), (4, C4 / C1)):
            pair = (X(4 + k) + X(4 - k)) + (z(k) + z(-k))
            total = pair if a is None else total + a * pair
        return total

    def neighbours(ref, pre, row, stored):
        z = lambda k: ref[pre + (OWN, rows(row + k), slice(None))]
        if stored:
            X = lambda k: ref[pre + (slice(k, k + 8), rows(row), slice(None))]
            return X, z
        c = z(0)
        wide_c = jnp.concatenate([up_lane(c[4:]), c, down_lane(c[:4])], axis=0)
        return (lambda k: wide_c[k : k + 8]), z

    def advance(field, s, centre, total, hi, m, injected, pulse):
        at = rows(m)
        if field == 0:
            return AS[:, at, :] * centre - hi + (VS[:, at, :] * total + pulse * G[s, :, at, :])
        return AR[:, at, :] * centre - D[:, at, :] * hi + VR[:, at, :] * (total + injected)

    def put_field(ref, pre, row, value):
        at = rows(row)
        ref[pre + (OWN, at, slice(None))] = value
        ref[pre + (slice(12, 16), at, slice(None))] = down_lane(value[:4])
        ref[pre + (slice(0, 4), at, slice(None))] = up_lane(value[4:])

    def first_step(slot, b, s, field, g, pulse, stored):
        p, m = 2 * s + field, 8 * g
        X, z = neighbours(N, (slot, p), m + 4, stored)
        injected = IA[s, b, :, rows(m), :] if field else None
        new = advance(field, s, z(0), spread(X, z), M[p, OWN, rows(m), :], m, injected, pulse)
        put_field(M, (p,), m, new)

    def second_step(slot, to, b, s, field, g, pulse, final=False):
        p, m = 2 * s + field, 8 * g + 4
        X, z = neighbours(M, (p,), m, True)
        injected = IB[s, b, :, rows(8 * g), :] if field else None
        hi = N[slot, p, OWN, rows(8 * g + 8), :]
        centre = z(0)
        new = advance(field, s, centre, spread(X, z), hi, m, injected, pulse)
        if final:
            N[to, p, OWN, rows(8 * g + 8), :] = new
        else:
            put_field(N, (to, p), 8 * g + 8, new)
            if field:
                CORR[:, rows(8 * g), :] += (
                    N[slot, p - 1, OWN, rows(8 * g + 8), :] * hi
                    + M[p - 1, OWN, rows(m), :] * centre
                )

    groups = depth // 8

    def pulse_of(s, step):
        return wavelet[start_step[s] + steps - 1 - step]

    def arrive_now(slot, p):
        def act(out, inn):
            now_copy(slot, p, out).wait_send()
            now_copy(slot, p, inn).wait_recv()

        return act

    def send_now(slot, p):
        def act(out, _):
            now_copy(slot, p, out).start()

        return act

    def arrive_raw(copies):
        def act(out, inn):
            for copy in copies:
                copy(out).wait_send()
                copy(inn).wait_recv()

        return act

    def edge_model(t):
        cols = slice(128 * t, 128 * (t + 1))
        return jnp.concatenate([RV[:, cols], 1.0 - 0.06 * RS[:, cols].astype(F32)], axis=0)

    def put_edge_model(r, value):
        V[r, 0:4, :] = value[0:4]
        V[r, 4 + depth : 8 + depth, :] = value[8:12]
        D[r, 0:4, :] = value[16:20]
        D[r, 4 + depth : 8 + depth, :] = value[24:28]

    def edge_rows(field):
        def block(t):
            cols = slice(128 * t, 128 * (t + 1))
            return jnp.concatenate([R[2 * s + field, :, cols] for s in range(shots)], axis=0)

        def put(r, value):
            for s in range(shots):
                p, at = 2 * s + field, 32 * s
                N[0, p, 4 + r, 0:8, :] = value[at : at + 8]
                M[p, 4 + r, 0:4, :] = value[at + 8 : at + 12]
                N[0, p, 4 + r, 8 + depth : 16 + depth, :] = value[at + 16 : at + 24]
                M[p, 4 + r, 4 + depth : 8 + depth, :] = value[at + 24 : at + 28]

        to_registers(block, 32 * shots, 1, put)

    for g in range(1, groups):
        coefficients(8 * g)
    for g in range(groups):
        CORR[:, rows(8 * g), :] = zeros
    each_way(arrive_raw([functools.partial(raw_model, 0), functools.partial(raw_model, 1)]))
    to_registers(edge_model, 32, 0, put_edge_model)
    coefficients(0)
    coefficients(8 * groups)

    def first_edges(field):
        for s in range(shots):
            for g in (1, groups - 1):
                first_step(0, 0, s, field, g, pulse_of(s, 0), True)
        for s in range(shots):
            p = 2 * s + field
            each_way(arrive_raw([functools.partial(raw_now, p), functools.partial(raw_hi, p)]))
        edge_rows(field)
        for s in range(shots):
            for g in (0, groups):
                first_step(0, 0, s, field, g, pulse_of(s, 0), False)
            for g in (0, groups - 1):
                second_step(0, 1, 0, s, field, g, pulse_of(s, 1))
            each_way(send_now(1, 2 * s + field))

    first_edges(0)
    field_in(1)
    tables()
    for s in range(shots):
        inject(s, 0)
    first_edges(1)
    for s in range(shots):
        for field in range(2):
            for g in range(2, groups - 1):
                first_step(0, 0, s, field, g, pulse_of(s, 0), True)

    def edges(b, slot, to, s, field, pulses):
        p = 2 * s + field
        each_way(arrive_now(slot, p))
        for g in (0, groups):
            first_step(slot, b, s, field, g, pulses[0], False)
        for g in (0, groups - 1):
            second_step(slot, to, b, s, field, g, pulses[1])
        each_way(send_now(to, p))

    def inner(b, slot, to, s, pulses, products=False):
        for field in range(2):
            for g in range(1, groups - 1):
                second_step(slot, to, b, s, field, g, pulses[1])
        if products:
            inject(s, b + 1)
        for field in range(2):
            for g in range(1, groups):
                first_step(to, b + 1, s, field, g, pulses[2], True)

    def pulses_of(s, b):
        return [pulse_of(s, 2 * b + j) for j in range(3)]

    for s in range(shots):
        inner(0, 0, 1, s, pulses_of(s, 0))

    def two_blocks(i, carry):
        for e in range(2):
            b, slot, to = 2 * i + 1 + e, 1 - e, e
            for s in range(shots):
                pulses = pulses_of(s, b)
                for field in range(2):
                    edges(b, slot, to, s, field, pulses)
                inner(b, slot, to, s, pulses, e == 0)
        return carry

    lax.fori_loop(0, blocks // 2 - 1, two_blocks, 0)

    last = blocks - 1
    slot, to = 1, 0
    for g in range(groups):
        total = CORR[:, rows(8 * g), :]
        for s in range(shots):
            at = rows(8 * g + 8)
            total = total + N[slot, 2 * s, OWN, at, :] * N[slot, 2 * s + 1, OWN, at, :]
            at = rows(8 * g + 4)
            product = M[2 * s, OWN, at, :] * M[2 * s + 1, OWN, at, :]
            if g == 0:
                product = jnp.where(row8 < 4, 0.0, product)
            if g == groups - 1:
                product = jnp.where(row8 < 4, product, 0.0)
            total = total + product
        CORR[:, rows(8 * g), :] = total

    def remote(src, dst, send, recv, shot):
        return pltpu.make_async_remote_copy(
            src_ref=src,
            dst_ref=dst,
            send_sem=send,
            recv_sem=recv,
            device_id={"shot": shot},
            device_id_type=MESH,
        )

    mine = pl.ds(4 * core, 4)
    pair = remote(CORR.at[pl.ds(4 * (1 - core), 4)], PAIR, pair_send.at[0], pair_recv.at[0], partner)
    pair.start()

    def final_step(wanted):
        for s in range(shots):
            for field in range(2):
                for g in wanted:
                    second_step(slot, to, last, s, field, g, pulse_of(s, steps - 1), True)

    final_step(range(1, groups - 1))
    pair.wait()
    HALF[...] = CORR[mine] + PAIR[...]

    def scatter(d):
        other = lax.rem(chip + d, chips)
        return remote(
            HALF.at[:, pl.ds(other * part, part), :],
            PARTS.at[chips - d],
            rs_send.at[d],
            rs_recv.at[chips - d],
            other * 2 + core,
        )

    def scattered(d):
        return remote(HALF.at[:, pl.ds(0, part), :], PARTS.at[d], rs_send.at[d], rs_recv.at[d], partner)

    order = sorted(range(1, chips), key=lambda d: -min(d, chips - d))
    for d in order:
        scatter(d).start()

    for s in range(shots):
        for field in range(2):
            each_way(arrive_now(slot, 2 * s + field))
            for g in (0, groups):
                first_step(slot, last, s, field, g, pulse_of(s, 2 * last), False)

    late = zeros
    for s in range(shots):
        low, high = rows(4), rows(depth - 4)
        late = late + jnp.where(
            row8 < 4,
            M[2 * s, OWN, low, :] * M[2 * s + 1, OWN, low, :],
            M[2 * s, OWN, high, :] * M[2 * s + 1, OWN, high, :],
        )
    LATE[...] = late
    late_pair = remote(
        LATE.at[pl.ds(4 * (1 - core), 4)], LPAIR, pair_send.at[2], pair_recv.at[2], partner
    )
    late_pair.start()
    final_step((0, groups - 1))
    late_pair.wait()
    LHALF[...] = LATE[mine] + LPAIR[...]

    def spread_late(d):
        other = lax.rem(chip + d, chips)
        return remote(
            LHALF, LPARTS.at[chips - d], l_send.at[d], l_recv.at[chips - d], other * 2 + core
        )

    def late_from(d):
        return remote(LHALF, LPARTS.at[d], l_send.at[d], l_recv.at[d], partner)

    for d in order:
        spread_late(d).start()

    def from_registers(get, count, slot, put):
        for r in range(8):
            T[slot, pl.ds(r, 128, stride=8), 0:count] = get(r).T
        for t in range(8):
            put(t, T[slot, 128 * t : 128 * (t + 1), 0:count].T)

    def field_out(field, ref):
        def get(r):
            return jnp.concatenate(
                [N[to, 2 * s + field, 4 + r, 8 : 8 + depth, :] for s in range(shots)], axis=0
            )

        def put(t, value):
            for s in range(shots):
                ref[s, :, 128 * t : 128 * (t + 1)] = value[depth * s : depth * (s + 1)]

        from_registers(get, shots * depth, field, put)

    for d in order:
        scattered(d).wait_recv()
    total = HALF[:, pl.ds(chip * part, part), :]
    for d in range(1, chips):
        total = total + PARTS[d]
    FIN[...] = total * (1.0 / math.sqrt(steps * shots * members))

    def gather(d):
        other = lax.rem(chip + d, chips)
        return remote(
            FIN,
            IMG.at[mine, pl.ds(chip * part, part), :],
            ag_send.at[d],
            ag_recv.at[chips - d],
            other * 2 + core,
        )

    def gathered(d):
        other = lax.rem(chip + d, chips)
        return remote(
            FIN,
            IMG.at[mine, pl.ds(other * part, part), :],
            ag_send.at[d],
            ag_recv.at[d],
            partner,
        )

    for d in order:
        gather(d).start()
    IMG[mine, pl.ds(chip * part, part), :] = FIN[...]
    field_out(0, src_out)
    field_out(1, rec_out)
    for d in order:
        late_from(d).wait_recv()
    total = LHALF[...]
    for d in range(1, chips):
        total = total + LPARTS[d]
    LSUM[mine] = total * (1.0 / math.sqrt(steps * shots * members))
    late_swap = remote(LSUM.at[mine], LSUM.at[mine], pair_send.at[3], pair_recv.at[3], partner)
    late_swap.start()
    for d in order:
        gathered(d).wait_recv()
    swap = remote(IMG.at[mine], IMG.at[mine], pair_send.at[1], pair_recv.at[1], partner)
    swap.start()
    for d in range(1, chips):
        scatter(d).wait_send()
        gather(d).wait_send()
        spread_late(d).wait_send()
    late_swap.wait()
    swap.wait()

    for g in range(groups):
        value = IMG[:, rows(8 * g), :]
        if g == 0:
            value = value + jnp.where(row8 < 4, LSUM[...], 0.0)
        if g == groups - 1:
            value = value + jnp.where(row8 < 4, 0.0, LSUM[...])
        image_out[:, rows(8 * g), :] = value


def finish(image, src, rec, image_out, src_out, rec_out, T, natural, sem):
    copies = [
        pltpu.make_async_copy(src, src_out, sem.at[1]),
        pltpu.make_async_copy(rec, rec_out, sem.at[2]),
    ]
    for copy in copies:
        copy.start()
    depth = image.shape[1]
    for r in range(8):
        T[pl.ds(r, 128, stride=8), 0:depth] = image[r].T
    for t in range(8):
        natural[:, 128 * t : 128 * (t + 1)] = T[128 * t : 128 * (t + 1), 0:depth].T
    copies.append(pltpu.make_async_copy(natural, image_out, sem.at[0]))
    copies[-1].start()
    for copy in copies:
        copy.wait()


def local(
    courant_sq,
    sponge_level,
    source_later,
    source_now,
    receiver_later,
    receiver_now,
    traces,
    wavelet,
    source_depth,
    source_lateral,
    receiver_depth,
    receiver_lateral,
    checkpoint_step,
):
    depth, lateral = courant_sq.shape
    shots, steps, nrec = traces.shape
    members = lax.axis_size("shot")
    chips = members // 2
    part = depth // chips
    wide = depth + 8
    planes = 2 * shots
    vmem = pl.BlockSpec(memory_space=pltpu.VMEM)
    image, src_out, rec_out = pl.pallas_call(
        functools.partial(kernel, steps),
        name="rtm_window",
        out_shape=(
            jax.ShapeDtypeStruct((8, depth, 128), F32),
            jax.ShapeDtypeStruct((shots, depth, lateral), F32),
            jax.ShapeDtypeStruct((shots, depth, lateral), F32),
        ),
        in_specs=[pl.BlockSpec(memory_space=pltpu.HBM)] * 13,
        out_specs=(vmem, vmem, vmem),
        scratch_shapes=[
            pltpu.VMEM((depth, lateral), F32),
            pltpu.VMEM((depth, lateral), jnp.int32),
            *[pltpu.VMEM((shots, depth, lateral), F32) for _ in range(4)],
            pltpu.VMEM(traces.shape, F32),
            pltpu.VMEM(receiver_depth.shape, jnp.int32),
            pltpu.VMEM(receiver_lateral.shape, jnp.int32),
            pltpu.SMEM(wavelet.shape, F32),
            pltpu.SMEM(source_depth.shape, jnp.int32),
            pltpu.SMEM(source_lateral.shape, jnp.int32),
            pltpu.SMEM(checkpoint_step.shape, jnp.int32),
            pltpu.VMEM((planes, 32, lateral), F32),
            pltpu.VMEM((16, lateral), F32),
            pltpu.VMEM((16, lateral), jnp.int32),
            pltpu.SemaphoreType.DMA((13,)),
            pltpu.VMEM((2, planes, 16, depth + 16, 128), F32),
            pltpu.VMEM((planes, 16, wide, 128), F32),
            *[pltpu.VMEM((8, wide, 128), F32) for _ in range(6)],
            pltpu.VMEM((shots, 8, wide, 128), F32),
            pltpu.VMEM((shots, steps // 2, 8, wide, 128), F32),
            pltpu.VMEM((shots, steps // 2, 8, depth, 128), F32),
            pltpu.VMEM((shots, nrec, lateral), BF16),
            pltpu.VMEM((shots, wide, nrec), F32),
            pltpu.VMEM((2, lateral, 128), F32),
            pltpu.VMEM((8, depth, 128), F32),
            pltpu.VMEM((4, depth, 128), F32),
            pltpu.VMEM((4, depth, 128), F32),
            pltpu.VMEM((chips, 4, part, 128), F32),
            pltpu.VMEM((4, part, 128), F32),
            pltpu.VMEM((8, depth, 128), F32),
            pltpu.VMEM((8, 8, 128), F32),
            pltpu.VMEM((4, 8, 128), F32),
            pltpu.VMEM((4, 8, 128), F32),
            pltpu.VMEM((chips, 4, 8, 128), F32),
            pltpu.VMEM((8, 8, 128), F32),
            pltpu.SemaphoreType.DMA((planes, 2)),
            pltpu.SemaphoreType.DMA((2, planes, 2)),
            pltpu.SemaphoreType.DMA((planes, 2)),
            pltpu.SemaphoreType.DMA((planes, 2)),
            pltpu.SemaphoreType.DMA((2, 2)),
            pltpu.SemaphoreType.DMA((2, 2)),
            pltpu.SemaphoreType.DMA((4,)),
            pltpu.SemaphoreType.DMA((4,)),
            pltpu.SemaphoreType.DMA((chips,)),
            pltpu.SemaphoreType.DMA((chips,)),
            pltpu.SemaphoreType.DMA((chips,)),
            pltpu.SemaphoreType.DMA((chips,)),
            pltpu.SemaphoreType.DMA((chips,)),
            pltpu.SemaphoreType.DMA((chips,)),
        ],
        compiler_params=pltpu.CompilerParams(
            collective_id=0, has_side_effects=True, vmem_limit_bytes=VMEM_LIMIT
        ),
    )(
        *[
            pltpu.with_memory_space_constraint(x, pltpu.HBM)
            for x in (
                courant_sq,
                sponge_level,
                source_later,
                source_now,
                receiver_later,
                receiver_now,
                traces,
                receiver_depth,
                receiver_lateral,
                wavelet,
                source_depth,
                source_lateral,
                checkpoint_step,
            )
        ]
    )
    return pl.pallas_call(
        finish,
        name="finish",
        out_shape=(
            jax.ShapeDtypeStruct((depth, lateral), F32),
            jax.ShapeDtypeStruct((shots, depth, lateral), F32),
            jax.ShapeDtypeStruct((shots, depth, lateral), F32),
        ),
        in_specs=[vmem] * 3,
        out_specs=(pl.BlockSpec(memory_space=pltpu.HBM),) * 3,
        scratch_shapes=[
            pltpu.VMEM((lateral, 128), F32),
            pltpu.VMEM((depth, lateral), F32),
            pltpu.SemaphoreType.DMA((3,)),
        ],
        compiler_params=pltpu.CompilerParams(vmem_limit_bytes=VMEM_LIMIT),
    )(image, src_out, rec_out)


def solution(mesh):
    in_specs = (
        P(("grp", "slab"), None),
        P(("grp", "slab"), None),
        P(("grp", "shot"), "slab", None),
        P(("grp", "shot"), "slab", None),
        P(("grp", "shot"), "slab", None),
        P(("grp", "shot"), "slab", None),
        P(("grp", "shot"), None, None),
        P("grp"),
        P(("grp", "shot")),
        P(("grp", "shot")),
        P(("grp", "shot"), None),
        P(("grp", "shot"), None),
        P(("grp", "shot")),
    )
    out_specs = (
        P(("grp", "slab"), None),
        P(("grp", "shot"), "slab", None),
        P(("grp", "shot"), "slab", None),
    )
    return jax.shard_map(local, mesh=mesh, in_specs=in_specs, out_specs=out_specs, check_vma=False)
```

```python
import functools
import math

import jax
import jax.numpy as jnp
from jax import lax
from jax.experimental import pallas as pl
from jax.experimental.pallas import tpu as pltpu
from jax.sharding import PartitionSpec as P

MESH = pl.DeviceIdType.MESH
F32 = jnp.float32
BF16 = jnp.bfloat16
VMEM_LIMIT = 48 * 1024 * 1024

C0, C1, C2, C3, C4 = (-205.0 / 72.0, 8.0 / 5.0, -1.0 / 5.0, 8.0 / 315.0, -1.0 / 560.0)

OWN = slice(4, 12)


def rows(start, count=8):
    return pl.ds(start, count)


def kernel(
    steps,
    *refs,
):
    inputs, refs = refs[:13], refs[13:]
    (
        image_out,
        src_out,
        rec_out,
        courant,
        sponge,
        src_hi,
        src_now,
        rec_hi,
        rec_now,
        traces,
        rec_depth,
        rec_lateral,
        wavelet,
        src_depth,
        src_lateral,
        start_step,
        R,
        RV,
        RS,
        in_sem,
        N,
        M,
        V,
        D,
        AS,
        VS,
        AR,
        VR,
        G,
        IA0,
        IA1,
        IB0,
        IB1,
        W,
        DP,
        T,
        CORR,
        PAIR,
        HALF,
        PARTS,
        FIN,
        IMG,
        LATE,
        LPAIR,
        LHALF,
        LPARTS,
        LSUM,
        n_send,
        n_recv,
        h_send,
        h_recv,
        c_send,
        c_recv,
        pair_send,
        pair_recv,
        rs_send,
        rs_recv,
        ag_send,
        ag_recv,
        l_send,
        l_recv,
    ) = refs
    IA, IB = (IA0, IA1), (IB0, IB1)
    slab, slabs = lax.axis_index("slab"), lax.axis_size("slab")
    me, members = lax.axis_index("shot"), lax.axis_size("shot")
    chips = members // 2
    chip, core = me // 2, lax.rem(me, 2)
    depth = courant.shape[0]
    shots = src_now.shape[0]
    nrec = traces.shape[2]
    blocks = steps // 2
    wide = depth + 8
    first = slab * depth
    has_up, has_down = slab > 0, slab < slabs - 1
    part = depth // chips
    planes = 2 * shots

    barrier = pltpu.get_barrier_semaphore()

    def greet(target):
        pl.semaphore_signal(barrier, inc=1, device_id=target, device_id_type=MESH)

    @pl.when(has_up)
    def _():
        greet({"slab": slab - 1})

    @pl.when(has_down)
    def _():
        greet({"slab": slab + 1})

    partner = chip * 2 + (1 - core)
    greet({"shot": partner})
    peers = [lax.rem(chip + d, chips) * 2 + core for d in range(1, chips)]
    for peer in peers:
        greet({"shot": peer})

    local_refs = (
        courant, sponge, src_hi, src_now, rec_hi, rec_now, traces, rec_depth, rec_lateral,
        wavelet, src_depth, src_lateral, start_step,
    )
    loads = [
        pltpu.make_async_copy(inputs[i], local_refs[i], in_sem.at[i])
        for i in (0, 1, 3, 2, 5, 4, 9, 10, 11, 12, 6, 7, 8)
    ]
    for load in loads:
        load.start()

    lane = lax.broadcasted_iota(jnp.int32, (4, 8, 128), 2)
    lane8 = lax.broadcasted_iota(jnp.int32, (8, 8, 128), 2)
    reg8 = lax.broadcasted_iota(jnp.int32, (8, 8, 128), 0)
    row8 = lax.broadcasted_iota(jnp.int32, (8, 8, 128), 1)
    cell8 = 8 * lane8 + reg8

    def up_lane(v):
        return jnp.where(lane == 0, 0.0, pltpu.roll(v, 1, axis=2))

    def down_lane(v):
        return jnp.where(lane == 127, 0.0, pltpu.roll(v, 127, axis=2))

    def to_registers(block, count, slot, put):
        for t in range(8):
            T[slot, 128 * t : 128 * (t + 1), 0:count] = block(t).T
        for r in range(8):
            put(r, T[slot, pl.ds(r, 128, stride=8), 0:count].T)

    def field_block(ref):
        return lambda t: ref[:, :, 128 * t : 128 * (t + 1)].reshape(shots * depth, 128)

    def put_now(field):
        def put(r, value):
            for s in range(shots):
                v = value[depth * s : depth * (s + 1)]
                N[0, 2 * s + field, 4 + r, 8 : 8 + depth, :] = v
                edge = lax.broadcasted_iota(jnp.int32, (depth, 128), 1)
                if r < 4:
                    N[0, 2 * s + field, 12 + r, 8 : 8 + depth, :] = jnp.where(
                        edge == 127, 0.0, pltpu.roll(v, 127, axis=1)
                    )
                else:
                    N[0, 2 * s + field, r - 4, 8 : 8 + depth, :] = jnp.where(
                        edge == 0, 0.0, pltpu.roll(v, 1, axis=1)
                    )

        return put

    def put_hi(field):
        def put(r, value):
            for s in range(shots):
                M[2 * s + field, 4 + r, 4 : 4 + depth, :] = value[depth * s : depth * (s + 1)]

        return put

    def model_block(t):
        cols = slice(128 * t, 128 * (t + 1))
        return jnp.concatenate(
            [courant[:, cols], 1.0 - 0.06 * sponge[:, cols].astype(F32)], axis=0
        )

    def put_model(r, value):
        V[r, 4 : 4 + depth, :] = value[:depth]
        D[r, 4 : 4 + depth, :] = value[depth:]

    zeros = jnp.zeros((8, 8, 128), F32)

    def clear(side):
        for p in range(planes):
            R[p, 16 * side : 16 * (side + 1), :] = jnp.zeros((16, 1024), F32)
            for slot in range(2):
                N[slot, p, OWN, rows((8 + depth) * side), :] = zeros
        RV[8 * side : 8 * (side + 1), :] = jnp.zeros((8, 1024), F32)
        RS[8 * side : 8 * (side + 1), :] = jnp.zeros((8, 1024), jnp.int32)

    @pl.when(slab == 0)
    def _():
        clear(0)

    @pl.when(slab == slabs - 1)
    def _():
        clear(1)

    def shift(ref_at, src_row, dst_row, count, send, recv, to):
        return pltpu.make_async_remote_copy(
            src_ref=ref_at(src_row, count),
            dst_ref=ref_at(dst_row, count),
            send_sem=send,
            recv_sem=recv,
            device_id={"slab": to},
            device_id_type=MESH,
        )

    def now_copy(slot, p, direction):
        at = lambda row, count: N.at[slot, p, OWN, pl.ds(row, count), :]
        if direction == 0:
            return shift(at, 8, 8 + depth, 8, n_send.at[p, 0], n_recv.at[slot, p, 0], slab - 1)
        return shift(at, depth, 0, 8, n_send.at[p, 1], n_recv.at[slot, p, 1], slab + 1)

    fields = (src_now, src_hi), (rec_now, rec_hi)

    def raw(src, dst, send, recv, direction):
        return pltpu.make_async_remote_copy(
            src_ref=src,
            dst_ref=dst,
            send_sem=send,
            recv_sem=recv,
            device_id={"slab": slab - 1 if direction == 0 else slab + 1},
            device_id_type=MESH,
        )

    def raw_now(p, direction):
        row = 0 if direction == 0 else depth - 8
        return raw(
            fields[p % 2][0].at[p // 2, pl.ds(row, 8), :],
            R.at[p, pl.ds(16 * (1 - direction), 8), :],
            n_send.at[p, direction],
            n_recv.at[0, p, direction],
            direction,
        )

    def raw_hi(p, direction):
        row = 0 if direction == 0 else depth - 4
        return raw(
            fields[p % 2][1].at[p // 2, pl.ds(row, 4), :],
            R.at[p, pl.ds(16 * (1 - direction) + 8, 4), :],
            h_send.at[p, direction],
            h_recv.at[p, direction],
            direction,
        )

    def raw_model(which, direction):
        row = 0 if direction == 0 else depth - 4
        return raw(
            (courant, sponge)[which].at[pl.ds(row, 4), :],
            (RV, RS)[which].at[pl.ds(8 * (1 - direction), 4), :],
            c_send.at[which, direction],
            c_recv.at[which, direction],
            direction,
        )

    def each_way(act):
        @pl.when(has_up)
        def _():
            act(0, 1)

        @pl.when(has_down)
        def _():
            act(1, 0)

    greeted = (
        has_up.astype(jnp.int32) + has_down.astype(jnp.int32) + len(peers) + 1
    )
    pl.semaphore_wait(barrier, greeted)

    for load in loads[:6]:
        load.wait()

    def send_first(out, _):
        raw_model(0, out).start()
        raw_model(1, out).start()
        for field in range(2):
            for s in range(shots):
                raw_now(2 * s + field, out).start()
                raw_hi(2 * s + field, out).start()

    each_way(send_first)

    def field_in(field):
        to_registers(field_block(fields[field][0]), shots * depth, 1, put_now(field))
        to_registers(field_block(fields[field][1]), shots * depth, 0, put_hi(field))

    to_registers(model_block, shots * depth, 0, put_model)
    field_in(0)
    for load in loads[6:]:
        load.wait()

    pad = 16 * ((wide + 15) // 16)
    top = 2 * pad

    def tables():
        rec_ids = first - 4 + lax.broadcasted_iota(jnp.int32, (wide, nrec), 0)
        for s in range(shots):
            DP[s] = (rec_ids == rec_depth[s : s + 1, :]).astype(F32)
            for q in range(nrec // 128):
                wanted = jnp.broadcast_to(
                    rec_lateral[s : s + 1, 128 * q : 128 * (q + 1)].astype(F32), (128, 128)
                ).T
                at = lax.broadcasted_iota(jnp.int32, (128, 128), 1).astype(F32) * 8.0
                for r in range(8):
                    W[s, 128 * q : 128 * (q + 1), 128 * r : 128 * (r + 1)] = (
                        (wanted == at + float(r)).astype(F32).astype(BF16)
                    )

    def inject(s, parity, block):
        def terms(step):
            t = traces[s, pl.ds(step, 1), :] * (1.0 / C1)
            hi = t.astype(BF16).astype(F32)
            return hi, t - hi

        gap = jnp.zeros((pad - wide, nrec), F32)
        table = []
        for term in terms(2 * block):
            table += [DP[s] * term, gap]
        for term in terms(2 * block + 1):
            table += [DP[s, 4 : 4 + depth, :] * term]
        table = jnp.concatenate(table, axis=0).astype(BF16)
        for c in range(4):
            got = jnp.dot(table, W[s, :, 256 * c : 256 * (c + 1)], preferred_element_type=F32)
            a = got[0:wide] + got[pad : pad + wide]
            b = got[top : top + depth] + got[top + depth : top + 2 * depth]
            for h in range(2):
                IA[parity][s, 2 * c + h] = a[:, 128 * h : 128 * (h + 1)]
                IB[parity][s, 2 * c + h] = b[:, 128 * h : 128 * (h + 1)]

    def coefficients(m):
        at = rows(m)
        v, d = V[:, at, :], D[:, at, :]
        a = 2.0 + (2.0 * C0) * v
        AS[:, at, :] = a
        AR[:, at, :] = d * a
        VS[:, at, :] = C1 * v
        VR[:, at, :] = (C1 * d) * v
        for s in range(shots):
            hit = (cell8 == src_lateral[s]) & (row8 + (first - 4 + m) == src_depth[s])
            G[s, :, at, :] = jnp.where(hit, -v, 0.0)

    def spread(X, z):
        total = None
        for k, a in ((1, None), (2, C2 / C1), (3, C3 / C1), (4, C4 / C1)):
            pair = (X(4 + k) + X(4 - k)) + (z(k) + z(-k))
            total = pair if a is None else total + a * pair
        return total

    def neighbours(ref, pre, row, stored):
        z = lambda k: ref[pre + (OWN, rows(row + k), slice(None))]
        if stored:
            X = lambda k: ref[pre + (slice(k, k + 8), rows(row), slice(None))]
            return X, z
        c = z(0)
        wide_c = jnp.concatenate([up_lane(c[4:]), c, down_lane(c[:4])], axis=0)
        return (lambda k: wide_c[k : k + 8]), z

    def advance(field, s, centre, total, hi, m, injected, pulse):
        at = rows(m)
        if field == 0:
            return AS[:, at, :] * centre - hi + (VS[:, at, :] * total + pulse * G[s, :, at, :])
        return AR[:, at, :] * centre - D[:, at, :] * hi + VR[:, at, :] * (total + injected)

    def put_field(ref, pre, row, value):
        at = rows(row)
        ref[pre + (OWN, at, slice(None))] = value
        ref[pre + (slice(12, 16), at, slice(None))] = down_lane(value[:4])
        ref[pre + (slice(0, 4), at, slice(None))] = up_lane(value[4:])

    def first_step(slot, b, s, field, g, pulse, stored):
        p, m = 2 * s + field, 8 * g
        X, z = neighbours(N, (slot, p), m + 4, stored)
        injected = IA[b][s, :, rows(m), :] if field else None
        new = advance(field, s, z(0), spread(X, z), M[p, OWN, rows(m), :], m, injected, pulse)
        put_field(M, (p,), m, new)

    def second_step(slot, to, b, s, field, g, pulse, final=False):
        p, m = 2 * s + field, 8 * g + 4
        X, z = neighbours(M, (p,), m, True)
        injected = IB[b][s, :, rows(8 * g), :] if field else None
        hi = N[slot, p, OWN, rows(8 * g + 8), :]
        centre = z(0)
        new = advance(field, s, centre, spread(X, z), hi, m, injected, pulse)
        if final:
            N[to, p, OWN, rows(8 * g + 8), :] = new
        else:
            put_field(N, (to, p), 8 * g + 8, new)
            if field:
                CORR[:, rows(8 * g), :] += (
                    N[slot, p - 1, OWN, rows(8 * g + 8), :] * hi
                    + M[p - 1, OWN, rows(m), :] * centre
                )

    groups = depth // 8

    def pulse_of(s, step):
        return wavelet[start_step[s] + steps - 1 - step]

    def arrive_now(slot, p):
        def act(out, inn):
            now_copy(slot, p, out).wait_send()
            now_copy(slot, p, inn).wait_recv()

        return act

    def send_now(slot, p):
        def act(out, _):
            now_copy(slot, p, out).start()

        return act

    def arrive_raw(copies):
        def act(out, inn):
            for copy in copies:
                copy(out).wait_send()
                copy(inn).wait_recv()

        return act

    def edge_model(t):
        cols = slice(128 * t, 128 * (t + 1))
        return jnp.concatenate([RV[:, cols], 1.0 - 0.06 * RS[:, cols].astype(F32)], axis=0)

    def put_edge_model(r, value):
        V[r, 0:4, :] = value[0:4]
        V[r, 4 + depth : 8 + depth, :] = value[8:12]
        D[r, 0:4, :] = value[16:20]
        D[r, 4 + depth : 8 + depth, :] = value[24:28]

    def edge_rows(field):
        def block(t):
            cols = slice(128 * t, 128 * (t + 1))
            return jnp.concatenate([R[2 * s + field, :, cols] for s in range(shots)], axis=0)

        def put(r, value):
            for s in range(shots):
                p, at = 2 * s + field, 32 * s
                N[0, p, 4 + r, 0:8, :] = value[at : at + 8]
                M[p, 4 + r, 0:4, :] = value[at + 8 : at + 12]
                N[0, p, 4 + r, 8 + depth : 16 + depth, :] = value[at + 16 : at + 24]
                M[p, 4 + r, 4 + depth : 8 + depth, :] = value[at + 24 : at + 28]

        to_registers(block, 32 * shots, 1, put)

    for g in range(1, groups):
        coefficients(8 * g)
    for g in range(groups):
        CORR[:, rows(8 * g), :] = zeros
    each_way(arrive_raw([functools.partial(raw_model, 0), functools.partial(raw_model, 1)]))
    to_registers(edge_model, 32, 0, put_edge_model)
    coefficients(0)
    coefficients(8 * groups)

    def first_edges(field):
        for s in range(shots):
            for g in (1, groups - 1):
                first_step(0, 0, s, field, g, pulse_of(s, 0), True)
        for s in range(shots):
            p = 2 * s + field
            each_way(arrive_raw([functools.partial(raw_now, p), functools.partial(raw_hi, p)]))
        edge_rows(field)
        for s in range(shots):
            for g in (0, groups):
                first_step(0, 0, s, field, g, pulse_of(s, 0), False)
            for g in (0, groups - 1):
                second_step(0, 1, 0, s, field, g, pulse_of(s, 1))
        for s in range(shots):
            each_way(send_now(1, 2 * s + field))

    first_edges(0)
    field_in(1)
    tables()
    for s in range(shots):
        inject(s, 0, 0)
    first_edges(1)
    for s in range(shots):
        for field in range(2):
            for g in range(2, groups - 1):
                first_step(0, 0, s, field, g, pulse_of(s, 0), True)

    def edges(b, slot, to, s, field, pulses):
        p = 2 * s + field
        each_way(arrive_now(slot, p))
        for g in (0, groups):
            first_step(slot, slot, s, field, g, pulses[0], False)
        for g in (0, groups - 1):
            second_step(slot, to, slot, s, field, g, pulses[1])
        each_way(send_now(to, p))

    def inner(b, slot, to, s, pulses):
        inject(s, to, b + 1)
        for field in range(2):
            for g in range(1, groups - 1):
                second_step(slot, to, slot, s, field, g, pulses[1])
        for field in range(2):
            for g in range(1, groups):
                first_step(to, to, s, field, g, pulses[2], True)

    def pulses_of(s, b):
        return [pulse_of(s, 2 * b + j) for j in range(3)]

    for s in range(shots):
        inner(0, 0, 1, s, pulses_of(s, 0))

    def two_blocks(i, carry):
        for e in range(2):
            b, slot, to = 2 * i + 1 + e, 1 - e, e
            for s in range(shots):
                pulses = pulses_of(s, b)
                for field in range(2):
                    edges(b, slot, to, s, field, pulses)
                inner(b, slot, to, s, pulses)
        return carry

    lax.fori_loop(0, blocks // 2 - 1, two_blocks, 0)

    last = blocks - 1
    slot, to = 1, 0
    for g in range(groups):
        total = CORR[:, rows(8 * g), :]
        for s in range(shots):
            at = rows(8 * g + 8)
            total = total + N[slot, 2 * s, OWN, at, :] * N[slot, 2 * s + 1, OWN, at, :]
            at = rows(8 * g + 4)
            product = M[2 * s, OWN, at, :] * M[2 * s + 1, OWN, at, :]
            if g == 0:
                product = jnp.where(row8 < 4, 0.0, product)
            if g == groups - 1:
                product = jnp.where(row8 < 4, product, 0.0)
            total = total + product
        CORR[:, rows(8 * g), :] = total

    def remote(src, dst, send, recv, shot):
        return pltpu.make_async_remote_copy(
            src_ref=src,
            dst_ref=dst,
            send_sem=send,
            recv_sem=recv,
            device_id={"shot": shot},
            device_id_type=MESH,
        )

    mine = pl.ds(4 * core, 4)
    pair = remote(CORR.at[pl.ds(4 * (1 - core), 4)], PAIR, pair_send.at[0], pair_recv.at[0], partner)
    pair.start()

    def final_step(wanted):
        for s in range(shots):
            for field in range(2):
                for g in wanted:
                    second_step(slot, to, slot, s, field, g, pulse_of(s, steps - 1), True)

    final_step(range(1, groups - 1))
    pair.wait()
    HALF[...] = CORR[mine] + PAIR[...]

    def scatter(d):
        other = lax.rem(chip + d, chips)
        return remote(
            HALF.at[:, pl.ds(other * part, part), :],
            PARTS.at[chips - d],
            rs_send.at[d],
            rs_recv.at[chips - d],
            other * 2 + core,
        )

    def scattered(d):
        return remote(HALF.at[:, pl.ds(0, part), :], PARTS.at[d], rs_send.at[d], rs_recv.at[d], partner)

    order = sorted(range(1, chips), key=lambda d: -min(d, chips - d))
    for d in order:
        scatter(d).start()

    for s in range(shots):
        for field in range(2):
            each_way(arrive_now(slot, 2 * s + field))
            for g in (0, groups):
                first_step(slot, slot, s, field, g, pulse_of(s, 2 * last), False)

    late = zeros
    for s in range(shots):
        low, high = rows(4), rows(depth - 4)
        late = late + jnp.where(
            row8 < 4,
            M[2 * s, OWN, low, :] * M[2 * s + 1, OWN, low, :],
            M[2 * s, OWN, high, :] * M[2 * s + 1, OWN, high, :],
        )
    LATE[...] = late
    late_pair = remote(
        LATE.at[pl.ds(4 * (1 - core), 4)], LPAIR, pair_send.at[2], pair_recv.at[2], partner
    )
    late_pair.start()
    final_step((0, groups - 1))
    late_pair.wait()
    LHALF[...] = LATE[mine] + LPAIR[...]

    def spread_late(d):
        other = lax.rem(chip + d, chips)
        return remote(
            LHALF, LPARTS.at[chips - d], l_send.at[d], l_recv.at[chips - d], other * 2 + core
        )

    def late_from(d):
        return remote(LHALF, LPARTS.at[d], l_send.at[d], l_recv.at[d], partner)

    for d in order:
        spread_late(d).start()

    def from_registers(get, count, slot, put):
        for r in range(8):
            T[slot, pl.ds(r, 128, stride=8), 0:count] = get(r).T
        for t in range(8):
            put(t, T[slot, 128 * t : 128 * (t + 1), 0:count].T)

    def field_out(field, ref):
        def get(r):
            return jnp.concatenate(
                [N[to, 2 * s + field, 4 + r, 8 : 8 + depth, :] for s in range(shots)], axis=0
            )

        def put(t, value):
            for s in range(shots):
                ref[s, :, 128 * t : 128 * (t + 1)] = value[depth * s : depth * (s + 1)]

        from_registers(get, shots * depth, field, put)

    for d in order:
        scattered(d).wait_recv()
    total = HALF[:, pl.ds(chip * part, part), :]
    for d in range(1, chips):
        total = total + PARTS[d]
    FIN[...] = total * (1.0 / math.sqrt(steps * shots * members))

    def gather(d):
        other = lax.rem(chip + d, chips)
        return remote(
            FIN,
            IMG.at[mine, pl.ds(chip * part, part), :],
            ag_send.at[d],
            ag_recv.at[chips - d],
            other * 2 + core,
        )

    def gathered(d):
        other = lax.rem(chip + d, chips)
        return remote(
            FIN,
            IMG.at[mine, pl.ds(other * part, part), :],
            ag_send.at[d],
            ag_recv.at[d],
            partner,
        )

    for d in order:
        gather(d).start()
    IMG[mine, pl.ds(chip * part, part), :] = FIN[...]
    field_out(0, src_out)
    field_out(1, rec_out)
    for d in order:
        late_from(d).wait_recv()
    total = LHALF[...]
    for d in range(1, chips):
        total = total + LPARTS[d]
    LSUM[mine] = total * (1.0 / math.sqrt(steps * shots * members))
    late_swap = remote(LSUM.at[mine], LSUM.at[mine], pair_send.at[3], pair_recv.at[3], partner)
    late_swap.start()
    for d in order:
        gathered(d).wait_recv()
    swap = remote(IMG.at[mine], IMG.at[mine], pair_send.at[1], pair_recv.at[1], partner)
    swap.start()
    for d in range(1, chips):
        scatter(d).wait_send()
        gather(d).wait_send()
        spread_late(d).wait_send()
    late_swap.wait()
    swap.wait()

    for g in range(groups):
        value = IMG[:, rows(8 * g), :]
        if g == 0:
            value = value + jnp.where(row8 < 4, LSUM[...], 0.0)
        if g == groups - 1:
            value = value + jnp.where(row8 < 4, 0.0, LSUM[...])
        image_out[:, rows(8 * g), :] = value


def finish(image, src, rec, image_out, src_out, rec_out, T, natural, sem):
    copies = [
        pltpu.make_async_copy(src, src_out, sem.at[1]),
        pltpu.make_async_copy(rec, rec_out, sem.at[2]),
    ]
    for copy in copies:
        copy.start()
    depth = image.shape[1]
    for r in range(8):
        T[pl.ds(r, 128, stride=8), 0:depth] = image[r].T
    for t in range(8):
        natural[:, 128 * t : 128 * (t + 1)] = T[128 * t : 128 * (t + 1), 0:depth].T
    copies.append(pltpu.make_async_copy(natural, image_out, sem.at[0]))
    copies[-1].start()
    for copy in copies:
        copy.wait()


def local(
    courant_sq,
    sponge_level,
    source_later,
    source_now,
    receiver_later,
    receiver_now,
    traces,
    wavelet,
    source_depth,
    source_lateral,
    receiver_depth,
    receiver_lateral,
    checkpoint_step,
):
    depth, lateral = courant_sq.shape
    shots, steps, nrec = traces.shape
    members = lax.axis_size("shot")
    chips = members // 2
    part = depth // chips
    wide = depth + 8
    planes = 2 * shots
    vmem = pl.BlockSpec(memory_space=pltpu.VMEM)
    image, src_out, rec_out = pl.pallas_call(
        functools.partial(kernel, steps),
        name="rtm_window",
        out_shape=(
            jax.ShapeDtypeStruct((8, depth, 128), F32),
            jax.ShapeDtypeStruct((shots, depth, lateral), F32),
            jax.ShapeDtypeStruct((shots, depth, lateral), F32),
        ),
        in_specs=[pl.BlockSpec(memory_space=pltpu.HBM)] * 13,
        out_specs=(vmem, vmem, vmem),
        scratch_shapes=[
            pltpu.VMEM((depth, lateral), F32),
            pltpu.VMEM((depth, lateral), jnp.int32),
            *[pltpu.VMEM((shots, depth, lateral), F32) for _ in range(4)],
            pltpu.VMEM(traces.shape, F32),
            pltpu.VMEM(receiver_depth.shape, jnp.int32),
            pltpu.VMEM(receiver_lateral.shape, jnp.int32),
            pltpu.SMEM(wavelet.shape, F32),
            pltpu.SMEM(source_depth.shape, jnp.int32),
            pltpu.SMEM(source_lateral.shape, jnp.int32),
            pltpu.SMEM(checkpoint_step.shape, jnp.int32),
            pltpu.VMEM((planes, 32, lateral), F32),
            pltpu.VMEM((16, lateral), F32),
            pltpu.VMEM((16, lateral), jnp.int32),
            pltpu.SemaphoreType.DMA((13,)),
            pltpu.VMEM((2, planes, 16, depth + 16, 128), F32),
            pltpu.VMEM((planes, 16, wide, 128), F32),
            *[pltpu.VMEM((8, wide, 128), F32) for _ in range(6)],
            pltpu.VMEM((shots, 8, wide, 128), F32),
            *[pltpu.VMEM((shots, 8, wide, 128), F32) for _ in range(2)],
            *[pltpu.VMEM((shots, 8, depth, 128), F32) for _ in range(2)],
            pltpu.VMEM((shots, nrec, lateral), BF16),
            pltpu.VMEM((shots, wide, nrec), F32),
            pltpu.VMEM((2, lateral, 128), F32),
            pltpu.VMEM((8, depth, 128), F32),
            pltpu.VMEM((4, depth, 128), F32),
            pltpu.VMEM((4, depth, 128), F32),
            pltpu.VMEM((chips, 4, part, 128), F32),
            pltpu.VMEM((4, part, 128), F32),
            pltpu.VMEM((8, depth, 128), F32),
            pltpu.VMEM((8, 8, 128), F32),
            pltpu.VMEM((4, 8, 128), F32),
            pltpu.VMEM((4, 8, 128), F32),
            pltpu.VMEM((chips, 4, 8, 128), F32),
            pltpu.VMEM((8, 8, 128), F32),
            pltpu.SemaphoreType.DMA((planes, 2)),
            pltpu.SemaphoreType.DMA((2, planes, 2)),
            pltpu.SemaphoreType.DMA((planes, 2)),
            pltpu.SemaphoreType.DMA((planes, 2)),
            pltpu.SemaphoreType.DMA((2, 2)),
            pltpu.SemaphoreType.DMA((2, 2)),
            pltpu.SemaphoreType.DMA((4,)),
            pltpu.SemaphoreType.DMA((4,)),
            pltpu.SemaphoreType.DMA((chips,)),
            pltpu.SemaphoreType.DMA((chips,)),
            pltpu.SemaphoreType.DMA((chips,)),
            pltpu.SemaphoreType.DMA((chips,)),
            pltpu.SemaphoreType.DMA((chips,)),
            pltpu.SemaphoreType.DMA((chips,)),
        ],
        compiler_params=pltpu.CompilerParams(
            collective_id=0, has_side_effects=True, vmem_limit_bytes=VMEM_LIMIT
        ),
    )(
        *[
            pltpu.with_memory_space_constraint(x, pltpu.HBM)
            for x in (
                courant_sq,
                sponge_level,
                source_later,
                source_now,
                receiver_later,
                receiver_now,
                traces,
                receiver_depth,
                receiver_lateral,
                wavelet,
                source_depth,
                source_lateral,
                checkpoint_step,
            )
        ]
    )
    return pl.pallas_call(
        finish,
        name="finish",
        out_shape=(
            jax.ShapeDtypeStruct((depth, lateral), F32),
            jax.ShapeDtypeStruct((shots, depth, lateral), F32),
            jax.ShapeDtypeStruct((shots, depth, lateral), F32),
        ),
        in_specs=[vmem] * 3,
        out_specs=(pl.BlockSpec(memory_space=pltpu.HBM),) * 3,
        scratch_shapes=[
            pltpu.VMEM((lateral, 128), F32),
            pltpu.VMEM((depth, lateral), F32),
            pltpu.SemaphoreType.DMA((3,)),
        ],
        compiler_params=pltpu.CompilerParams(vmem_limit_bytes=VMEM_LIMIT),
    )(image, src_out, rec_out)


def solution(mesh):
    in_specs = (
        P(("grp", "slab"), None),
        P(("grp", "slab"), None),
        P(("grp", "shot"), "slab", None),
        P(("grp", "shot"), "slab", None),
        P(("grp", "shot"), "slab", None),
        P(("grp", "shot"), "slab", None),
        P(("grp", "shot"), None, None),
        P("grp"),
        P(("grp", "shot")),
        P(("grp", "shot")),
        P(("grp", "shot"), None),
        P(("grp", "shot"), None),
        P(("grp", "shot")),
    )
    out_specs = (
        P(("grp", "slab"), None),
        P(("grp", "shot"), "slab", None),
        P(("grp", "shot"), "slab", None),
    )
    return jax.shard_map(local, mesh=mesh, in_specs=in_specs, out_specs=out_specs, check_vma=False)
```
